256 devices in a mesh: grp: 2 (over core), tile: 128 (over z, y, x).
Axes of the slice: x: 4, y: 4, z: 8, core: 2. Of those that a mesh axis runs over, the one named last changes fastest.
Arguments:
- source_points: float32 [2, 3, 4194304], P('grp', None, 'tile'), may hold values from -6 to 6
- intersection: int32 [2, 16384, 1], P('grp', 'tile'), may hold values from 0 to 127; in each aligned block of 128 rows (0 to 127, 128 to 255, ..., all dimensions but the last counted through in order) at most 2 rows name the same one
- target_scan: int32 [2, 16384], P('grp', 'tile'), may hold values from 0 to 63
- matches: int32 [2, 4194304], P('grp', 'tile'), may hold values from 0 to 511
- target_points: float32 [3, 4194304], P(None, 'tile'), may hold values from -6 to 6
- target_normals: float32 [3, 4194304], P(None, 'tile'), may hold values from -4 to 4
Outputs:
- pose_step: float32 [6, 8192], P(None, 'tile')
The draws below stay inside these ranges and needn't reach their ends.
Inputs may be any that keep to these rules, and one draw needn't show every extreme that they name: `intersection`: within the blocks of one device (each aligned run of 128 rows), no index is named more than 2 times, a bound that some block reaches.
All inputs are finite; a program needn't handle non-finite values.
Results may differ from the reference program's by a relative error of at most 0.0003.
Values sent between devices are 32-bit elements; how exact they have to be, the bound alone decides.
A program may use at most 64 MiB of HBM per device.

```python
import math
import jax
import jax.numpy as jnp
import numpy as np
from jax import lax

BLOCK_PTS = 256
BLOCKS_DEV = 128
SCANS_DEV = 64
TARGET_PTS = 512
CAP = 2
GRPS = 2
BLOCKS = 16384
SCANS = 8192
TILE_PTS = 4194304
N_TILE = 128


def set_ends(array, stream_key, least, top_value):
    longest = array.shape.index(max(array.shape))
    spots = []
    for shift in (0, 1):
        where = [jax.random.randint(jax.random.fold_in(stream_key, axis), (), 0, length) for axis, length in enumerate(array.shape)]
        where[longest] = (where[longest] + shift) % array.shape[longest]
        spots.append(tuple(where))
    return array.at[spots[0]].set(least).at[spots[1]].set(top_value)


def shard_levels(stream_key, shape, shards, smallest, high):
    def one(axis_at, parts):
        steps = jax.random.uniform(jax.random.fold_in(jax.random.fold_in(stream_key, 6), axis_at), (parts,), jnp.float32, smallest / len(shards), high / len(shards))
        return jnp.repeat(jnp.exp(steps), shape[axis_at] // parts).reshape((-1,) + (1,) * (len(shape) - axis_at - 1))

    level = one(*shards[0])
    for cut in shards[1:]:
        level = level * one(*cut)
    return level


def routed_block(own_key, own, number, rows, amount, top, limit, skew):
    order = jax.random.permutation(own_key, amount)
    crowded, usual = shares(amount, rows * top, limit, skew, True), shares(amount, rows * top, limit, skew, False)
    places = jnp.arange(amount)

    def named(tallies, rotation):
        used = int((tallies > 0).sum())
        fixed = max(1, used // 4)
        passed = fixed + (places - fixed + rotation * (used - fixed)) % max(1, amount - fixed)
        return jnp.zeros((amount,), jnp.int32).at[order[jnp.where(places < fixed, places, passed)]].set(jnp.asarray(tallies, jnp.int32))

    tallies = jnp.where(number % 4 == 0, named(crowded, number // 4), named(usual, number - number // 4 - 1))
    mixed = jax.random.permutation(jax.random.fold_in(own, 3), amount)
    source_of, sink = mixed[0:amount // 2 * 2:2], mixed[1:amount // 2 * 2:2]
    slack = jnp.minimum(tallies[source_of] - 1, limit - tallies[sink]) // 2
    slack = jnp.where((source_of == order[0]) | (sink == order[0]) | (tallies[sink] == 0), 0, jnp.maximum(slack, 0))
    passed = jax.random.randint(jax.random.fold_in(own, 4), (amount // 2,), 0, 1 << 20) % (slack + 1)
    tallies = tallies.at[source_of].add(-passed).at[sink].add(passed)
    members = jnp.searchsorted(jnp.cumsum(tallies), jnp.arange(rows * top), side="right").astype(jnp.int32)
    grid = members.reshape(top, rows).T
    grid = grid[jax.random.permutation(jax.random.fold_in(own, 1), rows)]
    rotation = jax.random.randint(jax.random.fold_in(own, 2), (rows, 1), 0, top)
    return jnp.take_along_axis(grid, (jnp.arange(top)[None, :] + rotation) % top, axis=1)


def shares(amount, total, most, lean, full):
    loads = [(1 << 20) // math.isqrt(grade ** lean) + 1 for grade in range(1, amount + 1)]
    largest = most if full else min(most, max(-(-total // amount), total * loads[0] // sum(loads)))
    least = 1 if total - largest >= amount - 1 else 0
    given, spare = [largest] + [least] * (amount - 1), total - largest - least * (amount - 1)
    while spare > 0:
        movable = [i for i in range(1, amount) if given[i] < largest] or [i for i in range(1, amount) if given[i] < most]
        pool, left = sum([loads[i] for i in movable]), spare
        for i in movable:
            more = min(most - given[i], max(1, left * loads[i] // pool), spare)
            given[i] = given[i] + more
            spare = spare - more
    return np.array(given)


def gaussian(key, extent, width, reach, pieces=(), kind=jnp.bfloat16):
    drawn = jax.random.normal(key, extent, jnp.float32) * width
    if len(pieces) > 0:
        drawn = shard_levels(key, extent, pieces, -0.22, 0.18) * drawn
    return jnp.clip(drawn, min=-reach, max=reach).astype(kind)


def setup_inputs(seed: int = 0) -> dict:
    keys = jax.random.split(jax.random.key(seed), 7)
    source_points = gaussian(keys[0], (GRPS, 3, BLOCKS * BLOCK_PTS), 1.0, 6.0, ((0, 2), (2, 128)), jnp.float32)
    intersection_keys = jax.random.split(jax.random.fold_in(keys[1], 1), GRPS * BLOCKS // BLOCKS_DEV)
    intersection_turns = jax.random.permutation(jax.random.fold_in(keys[1], 3), GRPS * BLOCKS // BLOCKS_DEV)
    intersection = jax.vmap(lambda own, number: routed_block(jax.random.fold_in(keys[1], 2), own, number, BLOCKS_DEV, N_TILE, 1, CAP, 2))(intersection_keys, intersection_turns).reshape((GRPS, BLOCKS, 1))
    target_scan = set_ends(jax.random.randint(keys[2], (GRPS, BLOCKS), 0, SCANS_DEV), jax.random.fold_in(keys[2], 1), 0, SCANS_DEV - 1).astype(jnp.int32)
    matches = set_ends(jax.random.randint(keys[3], (GRPS, BLOCKS * BLOCK_PTS), 0, TARGET_PTS), jax.random.fold_in(keys[3], 1), 0, TARGET_PTS - 1).astype(jnp.int32)
    target_points = gaussian(keys[4], (3, TILE_PTS), 1.0, 6.0, ((1, 128),), jnp.float32)
    target_normals = gaussian(keys[5], (3, TILE_PTS), 0.6, 4.0, ((1, 128),), jnp.float32)
    return {"source_points": source_points, "intersection": intersection, "target_scan": target_scan, "matches": matches, "target_points": target_points, "target_normals": target_normals}


DAMPING = 0.1
PRECISE = lax.Precision.HIGHEST


def cross_rows(first_vec, second_vec):
    return jnp.stack([first_vec[1] * second_vec[2] - first_vec[2] * second_vec[1],
                      first_vec[2] * second_vec[0] - first_vec[0] * second_vec[2],
                      first_vec[0] * second_vec[1] - first_vec[1] * second_vec[0]])


def pair_terms(source, target, normal, usable):
    jacobian = jnp.concatenate([cross_rows(source, normal), normal, -cross_rows(target, normal), -normal], axis=0) * usable[None]
    misfit = jnp.sum(normal * (source - target), axis=0) * usable
    normal_blocks = jnp.einsum("anks,bnks->abnk", jacobian, jacobian, precision=PRECISE)
    gradient = jnp.einsum("anks,nks->ank", jacobian, misfit, precision=PRECISE)
    layout = jacobian.shape[1:3]
    own_terms = jnp.concatenate([normal_blocks[:6, :6].reshape((36,) + layout), gradient[:6]], axis=0)
    theirs = jnp.concatenate([normal_blocks[6:, 6:].reshape((36,) + layout), gradient[6:]], axis=0)
    return own_terms, theirs


def solve_poses(scan_totals):
    entries = [[scan_totals[6 * row_at + col_at] for col_at in range(6)] for row_at in range(6)]
    traced = entries[0][0]
    for step_at in range(1, 6):
        traced = traced + entries[step_at][step_at]
    shift_by = DAMPING * traced / 6.0
    for step_at in range(6):
        entries[step_at][step_at] = entries[step_at][step_at] + shift_by
    values = [-scan_totals[36 + row_at] for row_at in range(6)]
    for pivot_at in range(6):
        for row_at in range(pivot_at + 1, 6):
            factor = entries[row_at][pivot_at] / entries[pivot_at][pivot_at]
            for col_at in range(pivot_at, 6):
                entries[row_at][col_at] = entries[row_at][col_at] - factor * entries[pivot_at][col_at]
            values[row_at] = values[row_at] - factor * values[pivot_at]
    result = [None] * 6
    for row_at in range(5, -1, -1):
        running = values[row_at]
        for col_at in range(row_at + 1, 6):
            running = running - entries[row_at][col_at] * result[col_at]
        result[row_at] = running / entries[row_at][row_at]
    return jnp.stack(result)


def reference(source_points, intersection, target_scan, matches, target_points, target_normals):
    per_scan = BLOCKS_DEV // SCANS_DEV
    block_span = BLOCKS_DEV * BLOCK_PTS
    tile_span = SCANS_DEV * TARGET_PTS
    anchor = jnp.int32(0)

    def accumulate(totals, stretch_at):
        grp_at = (stretch_at // N_TILE).astype(jnp.int32)
        tile_at = (stretch_at % N_TILE).astype(jnp.int32)
        coords = lax.dynamic_slice(source_points, (grp_at, anchor, tile_at * block_span), (1, 3, block_span))[0]
        coords = coords.reshape(3, 1, BLOCKS_DEV, BLOCK_PTS)
        destin = lax.dynamic_slice(intersection, (grp_at, tile_at * BLOCKS_DEV, anchor), (1, BLOCKS_DEV, 1))[0, :, 0]
        chosen = lax.dynamic_slice(target_scan, (grp_at, tile_at * BLOCKS_DEV), (1, BLOCKS_DEV))[0]
        picked = lax.dynamic_slice(matches, (grp_at, tile_at * block_span), (1, block_span))[0].reshape(BLOCKS_DEV, BLOCK_PTS)
        target_index = (destin[:, None] * tile_span + chosen[:, None] * TARGET_PTS + picked).astype(jnp.int32)
        nearest = jnp.take(target_points, target_index, axis=1)[:, None]
        facing = jnp.take(target_normals, target_index, axis=1)[:, None]
        usable = jnp.ones((1, BLOCKS_DEV, BLOCK_PTS), jnp.float32)
        own_terms, theirs = pair_terms(coords, nearest, facing, usable)
        source_ids = (tile_at * SCANS_DEV + jnp.arange(BLOCKS_DEV, dtype=jnp.int32) // per_scan).astype(jnp.int32)
        target_ids = (destin * SCANS_DEV + chosen).astype(jnp.int32)
        totals = totals + jax.ops.segment_sum(own_terms[:, 0].T, source_ids, num_segments=SCANS).T
        totals = totals + jax.ops.segment_sum(theirs[:, 0].T, target_ids, num_segments=SCANS).T
        return totals, None

    totals, unused = lax.scan(accumulate, jnp.zeros((42, SCANS), jnp.float32), jnp.arange(GRPS * N_TILE, dtype=jnp.int32))
    return solve_poses(totals)
```

```python
import jax
import jax.numpy as jnp
from jax import lax
from jax.experimental import pallas as pl
from jax.experimental.pallas import tpu as pltpu
from jax.sharding import PartitionSpec as P

TILES = 128
SCANS_DEV = 64
TARGET_PTS = 512
LANES = 128
DAMPING = 0.1
PRECISE = lax.Precision.HIGHEST
F32 = jnp.float32
I32 = jnp.int32
DZ_ORDER = (4, 3, 5, 2, 6, 1, 7, 0)

PAIRS = [(i, j) for i in range(3) for j in range(i, 3)]
AT_AN, AT_AM, AT_NN, AT_NM, AT_B = 6, 15, 18, 24, 32


def parts_of(value):
    high = value.astype(jnp.bfloat16)
    rest = value - high.astype(F32)
    middle = rest.astype(jnp.bfloat16)
    low = (rest - middle.astype(F32)).astype(jnp.bfloat16)
    return high, middle, low


def solve_rows(rows):
    entries = [[None] * 6 for _ in range(6)]
    for at, (i, j) in enumerate(PAIRS):
        entries[i][j] = entries[j][i] = rows[at]
        entries[3 + i][3 + j] = entries[3 + j][3 + i] = rows[AT_NN + at]
    for i in range(3):
        for j in range(3):
            entries[i][3 + j] = entries[3 + j][i] = rows[AT_AN + 3 * i + j]
    traced = entries[0][0]
    for at in range(1, 6):
        traced = traced + entries[at][at]
    shift_by = DAMPING * traced / 6.0
    for at in range(6):
        entries[at][at] = entries[at][at] + shift_by
    values = [-rows[AT_AM + i] for i in range(3)] + [-rows[AT_NM + i] for i in range(3)]
    for pivot in range(6):
        for row in range(pivot + 1, 6):
            factor = entries[row][pivot] / entries[pivot][pivot]
            for col in range(pivot + 1, 6):
                entries[row][col] = entries[row][col] - factor * entries[pivot][col]
            values[row] = values[row] - factor * values[pivot]
    result = [None] * 6
    for row in range(5, -1, -1):
        running = values[row]
        for col in range(row + 1, 6):
            running = running - entries[row][col] * result[col]
        result[row] = running / entries[row][row]
    return result


def cross(u, v):
    return [u[1] * v[2] - u[2] * v[1], u[2] * v[0] - u[0] * v[2], u[0] * v[1] - u[1] * v[0]]


def kernel(
    dest_hbm, scan_hbm, src_hbm, mat_hbm, tp_hbm, tn_hbm, out_ref,
    dest_v, scan_s, src_v, mat_v, tp_v, tn_v, inv_v, inv_s, table, rhs,
    send, recv, ucat, sums, ret_send, ret_recv, total, total_far,
    in_sem, inv_sem, send_sem, recv_sem, ret_ssem, ret_rsem, far_ssem, far_rsem,
):
    me_grp, me = lax.axis_index("grp"), lax.axis_index("tile")
    z, y, x = me // 16, (me // 4) % 4, me % 4

    barrier = pltpu.get_barrier_semaphore()

    def announce(at, carry):
        pl.semaphore_signal(barrier, 1, device_id={"tile": (me + at) % TILES})
        return carry

    pl.semaphore_signal(barrier, 1, device_id={"grp": 1 - me_grp})
    lax.fori_loop(1, TILES, announce, 0)

    copies = [
        pltpu.make_async_copy(s, d, in_sem.at[i])
        for i, (s, d) in enumerate(
            [(dest_hbm, dest_v), (scan_hbm, scan_s), (src_hbm, src_v), (mat_hbm, mat_v), (tp_hbm, tp_v), (tn_hbm, tn_v)]
        )
    ]
    for copy in copies:
        copy.start()

    copies[0].wait()
    blocks = jnp.broadcast_to(dest_v[...], (LANES, LANES)).T
    lane = lax.broadcasted_iota(I32, (LANES, LANES), 1)
    number = lax.broadcasted_iota(I32, (LANES, LANES), 0)
    named = blocks == lane
    first = jnp.min(jnp.where(named, number, 1000), axis=0, keepdims=True)
    last = jnp.max(jnp.where(named, number, -1), axis=0, keepdims=True)
    first = jnp.where(last < 0, -1, first)
    last = jnp.where(last == first, -1, last)
    inv_v[...] = jnp.concatenate([first, last], axis=0)
    to_smem = pltpu.make_async_copy(inv_v, inv_s, inv_sem)
    to_smem.start()
    for copy in copies[1:4]:
        copy.wait()
    to_smem.wait()

    def pack(d, carry):
        slots = send.at[pl.ds(pl.multiple_of(d * 16, 16), 16)]
        for r in range(2):
            l = inv_s[r, d]
            held = jnp.minimum(jnp.maximum(l, 0), TILES - 1)
            scale = jnp.where(l >= 0, 1, 0)
            base = jnp.where(l >= 0, scan_s[0, held] * TARGET_PTS, -1)
            for c in range(3):
                slots[r * 8 + 2 * c : r * 8 + 2 * c + 2, :] = src_v[c * TILES + held]
            slots[r * 8 + 6 : r * 8 + 8, :] = (mat_v[held] * scale + base).astype(F32)
        return carry

    lax.fori_loop(0, TILES, pack, 0, unroll=4)
    pl.semaphore_wait(barrier, TILES)

    def offset_of(group):
        return group % 4, group // 4

    def out_copy(group, j, dz):
        dx, dy = offset_of(group)
        to = ((z + dz) % 8) * 16 + ((y + dy) % 4) * 4 + (x + dx) % 4
        k = group * 8 + j
        return pltpu.make_async_remote_copy(
            src_ref=send.at[pl.ds(pl.multiple_of(to * 16, 16), 16)],
            dst_ref=recv.at[pl.ds(pl.multiple_of(k * 16, 16), 16)],
            send_sem=send_sem,
            recv_sem=recv_sem.at[group],
            device_id={"tile": to},
        )

    def issue(step, carry):
        group = 15 - step
        for j, dz in enumerate(DZ_ORDER):
            out_copy(group, j, dz).start()
        return carry

    lax.fori_loop(0, 15, issue, 0)
    for j, dz in enumerate(DZ_ORDER[:-1]):
        out_copy(0, j, dz).start()
    recv[7 * 16 : 8 * 16, :] = send[pl.ds(pl.multiple_of(me * 16, 16), 16), :]

    copies[4].wait()
    copies[5].wait()

    def spread(at, carry):
        rows = table.at[pl.ds(pl.multiple_of(at * 8, 8), 8)]
        columns = pl.ds(pl.multiple_of(at * LANES, LANES), LANES)
        rows[0:3, :] = tp_v[:, columns]
        rows[3:6, :] = tn_v[:, columns]
        return carry

    lax.fori_loop(0, 4 * SCANS_DEV, spread, 0, unroll=8)
    for c in range(6):
        for chunk in range(4):
            column = jnp.concatenate(
                [table[pl.ds((s8 * 32 + chunk) * 8 + c, 8, stride=32), :] for s8 in range(8)], axis=0
            )
            at = (c * 4 + chunk) * LANES
            for part, piece in enumerate(parts_of(column)):
                rhs[part * 64 : (part + 1) * 64, at : at + LANES] = piece

    lane8 = lax.broadcasted_iota(I32, (8, LANES), 1)

    def settle(group):
        base = group * LANES
        wanted = [
            [recv[pl.ds(base + r * 8 + 6 + h, 8, stride=16), :].astype(I32) for h in range(2)] for r in range(2)
        ]
        points = [
            [[recv[pl.ds(base + r * 8 + 2 * c + h, 8, stride=16), :] for c in range(3)] for h in range(2)]
            for r in range(2)
        ]
        scan = [lax.shift_right_arithmetic(wanted[r][0][:, 0:1], 9) for r in range(2)]
        column = lax.broadcasted_iota(I32, (8, 3 * SCANS_DEV), 1) & (SCANS_DEV - 1)
        picks = jnp.concatenate([jnp.where(column == scan[r], 1.0, 0.0) for r in range(2)], axis=0)
        picks = picks.astype(jnp.bfloat16)
        inside = [[wanted[r][h] & (LANES - 1) for h in range(2)] for r in range(2)]
        odd = [[(wanted[r][h] & LANES) != 0 for h in range(2)] for r in range(2)]
        upper = [[(wanted[r][h] & (2 * LANES)) != 0 for h in range(2)] for r in range(2)]
        found = [[[None] * 6 for _ in range(2)] for _ in range(2)]
        for c in range(6):
            held = jnp.dot(picks, rhs[:, c * TARGET_PTS : (c + 1) * TARGET_PTS], preferred_element_type=F32)
            for r in range(2):
                chunk = [held[r * 8 : r * 8 + 8, q * LANES : (q + 1) * LANES] for q in range(4)]
                for h in range(2):
                    got = [jnp.take_along_axis(chunk[q], inside[r][h], axis=1, mode="promise_in_bounds") for q in range(4)]
                    found[r][h][c] = jnp.where(
                        upper[r][h],
                        jnp.where(odd[r][h], got[3], got[2]),
                        jnp.where(odd[r][h], got[1], got[0]),
                    )
        result = jnp.zeros((8, LANES), F32)
        for r in range(2):
            terms = []
            for h in range(2):
                p, q, n = points[r][h], found[r][h][:3], found[r][h][3:]
                a, b = cross(p, n), cross(q, n)
                m = n[0] * (p[0] - q[0]) + n[1] * (p[1] - q[1]) + n[2] * (p[2] - q[2])
                terms.append((a, b, n, m))

            def summed(left, right):
                return jnp.sum(left(0) * right(0) + left(1) * right(1), axis=1, keepdims=True)

            def pick(which, i):
                return lambda h: terms[h][which] if i is None else terms[h][which][i]

            places = []
            for at, (i, j) in enumerate(PAIRS):
                places.append((at, pick(0, i), pick(0, j), 1))
                places.append((AT_NN + at, pick(2, i), pick(2, j), 1))
                places.append((AT_B + at, pick(1, i), pick(1, j), 1))
            for i in range(3):
                for j in range(3):
                    places.append((AT_AN + 3 * i + j, pick(0, i), pick(2, j), 1))
                    places.append((AT_B + AT_AN + 3 * i + j, pick(1, i), pick(2, j), 1))
                places.append((AT_AM + i, pick(0, i), pick(3, None), 1))
                places.append((AT_NM + i, pick(2, i), pick(3, None), 1))
                places.append((AT_B + AT_AM + i, pick(1, i), pick(3, None), -1))
            for at, left, right, sign in places:
                value = summed(left, right)
                result = jnp.where(lane8 == at + 64 * r, value if sign > 0 else -value, result)
        which = jnp.where(lane8 < 64, scan[0], scan[1])
        rows = pl.ds(pl.multiple_of(group * 8, 8), 8)
        ucat[rows, :] = jnp.where((lane8 & 63) == which, 1.0, 0.0)
        sums[rows, :] = result
        for i in range(8):
            ret_send[group * 8 + i] = result[i : i + 1, :]

    def back_copy(group, j, dz):
        dx, dy = offset_of(group)
        to = ((z + 8 - dz) % 8) * 16 + ((y + 4 - dy) % 4) * 4 + (x + 4 - dx) % 4
        return pltpu.make_async_remote_copy(
            src_ref=ret_send.at[group * 8 + j],
            dst_ref=ret_recv.at[me],
            send_sem=ret_ssem,
            recv_sem=ret_rsem,
            device_id={"tile": to},
        )

    def landed(first_row, rows, sem):
        return pltpu.make_async_copy(recv.at[pl.ds(first_row, rows)], recv.at[pl.ds(first_row, rows)], sem)

    def work(step, carry):
        group = 15 - step
        landed(pl.multiple_of(group * LANES, LANES), LANES, recv_sem.at[group]).wait()
        settle(group)
        for j, dz in enumerate(DZ_ORDER):
            back_copy(group, j, dz).start()
        return carry

    lax.fori_loop(0, 15, work, 0)
    landed(0, 7 * 16, recv_sem.at[0]).wait()
    settle(0)
    for j, dz in enumerate(DZ_ORDER[:-1]):
        back_copy(0, j, dz).start()
    ret_recv[me] = ret_send[7]

    by_target = jnp.dot(ucat[...].T, sums[...], precision=PRECISE, preferred_element_type=F32)
    by_target = by_target[:64] + pltpu.roll(by_target[64:], 64, axis=1)
    lane64 = lax.broadcasted_iota(I32, (SCANS_DEV, LANES), 1)
    moved = pltpu.roll(by_target, LANES - AT_B, axis=1)
    by_target = jnp.where(
        lane64 < AT_NN, moved, jnp.where(lane64 < AT_NM, by_target, jnp.where(lane64 < AT_NM + 3, -by_target, 0.0))
    )
    scan_row = lax.broadcasted_iota(I32, (SCANS_DEV, LANES), 0)
    owner = [lax.shift_right_arithmetic(inv_v[r : r + 1, :], 1) for r in range(2)]
    scat = jnp.concatenate([jnp.where(scan_row == owner[r], 1.0, 0.0) for r in range(2)], axis=0)

    others = ret_recv.at[pl.ds(0, TILES - 1)]
    pltpu.make_async_copy(others, others, ret_rsem).wait()
    returned = ret_recv[...].reshape(TILES, LANES)
    by_source = jnp.dot(scat, returned, precision=PRECISE, preferred_element_type=F32)
    by_source = by_source[:64] + pltpu.roll(by_source[64:], 64, axis=1)
    both = by_source + by_target
    flipped = jnp.concatenate([both, jnp.zeros_like(both)], axis=0).T
    total[...] = flipped[:32, :]
    far = pltpu.make_async_remote_copy(
        src_ref=total, dst_ref=total_far, send_sem=far_ssem, recv_sem=far_rsem, device_id={"grp": 1 - me_grp}
    )
    far.start()
    far.wait_recv()
    whole = total[...] + total_far[...]
    result = solve_rows([whole[at : at + 1, :] for at in range(27)])
    for row in range(6):
        out_ref[row : row + 1, :] = result[row][:, :SCANS_DEV]
    far.wait_send()
    ret_others = ret_send.at[pl.ds(0, TILES - 1)]
    pltpu.make_async_copy(ret_others, ret_others, ret_ssem).wait()
    sent = send.at[pl.ds(0, 16 * (TILES - 1))]
    pltpu.make_async_copy(sent, sent, send_sem).wait()


def body(source_points, intersection, target_scan, matches, target_points, target_normals):
    anywhere = pl.BlockSpec(memory_space=pl.ANY)
    vmem = pltpu.VMEM
    dma = pltpu.SemaphoreType.DMA
    return pl.pallas_call(
        kernel,
        name="icp_step",
        out_shape=jax.ShapeDtypeStruct((6, SCANS_DEV), F32),
        in_specs=[anywhere] * 6,
        out_specs=pl.BlockSpec(memory_space=pltpu.VMEM),
        scratch_shapes=[
            vmem((1, TILES), I32),
            pltpu.SMEM((1, TILES), I32),
            vmem((3 * TILES, 2, LANES), F32),
            vmem((TILES, 2, LANES), I32),
            vmem((3, SCANS_DEV * TARGET_PTS), F32),
            vmem((3, SCANS_DEV * TARGET_PTS), F32),
            vmem((2, TILES), I32),
            pltpu.SMEM((2, TILES), I32),
            vmem((SCANS_DEV * 4 * 8 + 32, LANES), F32),
            vmem((3 * SCANS_DEV, 6 * TARGET_PTS), jnp.bfloat16),
            vmem((TILES * 16, LANES), F32),
            vmem((TILES * 16 + 16, LANES), F32),
            vmem((TILES, LANES), F32),
            vmem((TILES, LANES), F32),
            vmem((TILES, 1, LANES), F32),
            vmem((TILES, 1, LANES), F32),
            vmem((32, LANES), F32),
            vmem((32, LANES), F32),
            dma((6,)),
            dma,
            dma,
            dma((16,)),
            dma,
            dma,
            dma,
            dma,
        ],
        compiler_params=pltpu.CompilerParams(collective_id=0, has_side_effects=True),
    )(
        intersection.reshape(1, TILES),
        target_scan,
        source_points.reshape(3 * TILES, 2, LANES),
        matches.reshape(TILES, 2, LANES),
        target_points,
        target_normals,
    )


def solution(mesh):
    in_specs = (
        P("grp", None, "tile"),
        P("grp", "tile", None),
        P("grp", "tile"),
        P("grp", "tile"),
        P(None, "tile"),
        P(None, "tile"),
    )
    return jax.shard_map(body, mesh=mesh, in_specs=in_specs, out_specs=P(None, "tile"), check_vma=False)
```

```python
import jax
import jax.numpy as jnp
from jax import lax
from jax.experimental import pallas as pl
from jax.experimental.pallas import tpu as pltpu
from jax.sharding import PartitionSpec as P

TILES = 128
SCANS_DEV = 64
TARGET_PTS = 512
LANES = 128
DAMPING = 0.1
PRECISE = lax.Precision.HIGHEST
F32 = jnp.float32
I32 = jnp.int32
DZ_ORDER = (4, 3, 5, 2, 6, 1, 7, 0)
PLANE = 16
LAG = 5
LEAD = 4

PAIRS = [(i, j) for i in range(3) for j in range(i, 3)]
AT_AN, AT_AM, AT_NN, AT_NM, AT_B = 6, 15, 18, 24, 32


def parts_of(value):
    high = value.astype(jnp.bfloat16)
    rest = value - high.astype(F32)
    middle = rest.astype(jnp.bfloat16)
    low = (rest - middle.astype(F32)).astype(jnp.bfloat16)
    return high, middle, low


def solve_rows(rows):
    entries = [[None] * 6 for _ in range(6)]
    for at, (i, j) in enumerate(PAIRS):
        entries[i][j] = entries[j][i] = rows[at]
        entries[3 + i][3 + j] = entries[3 + j][3 + i] = rows[AT_NN + at]
    for i in range(3):
        for j in range(3):
            entries[i][3 + j] = entries[3 + j][i] = rows[AT_AN + 3 * i + j]
    traced = entries[0][0]
    for at in range(1, 6):
        traced = traced + entries[at][at]
    shift_by = DAMPING * traced / 6.0
    for at in range(6):
        entries[at][at] = entries[at][at] + shift_by
    values = [-rows[AT_AM + i] for i in range(3)] + [-rows[AT_NM + i] for i in range(3)]
    for pivot in range(6):
        for row in range(pivot + 1, 6):
            factor = entries[row][pivot] / entries[pivot][pivot]
            for col in range(pivot + 1, 6):
                entries[row][col] = entries[row][col] - factor * entries[pivot][col]
            values[row] = values[row] - factor * values[pivot]
    result = [None] * 6
    for row in range(5, -1, -1):
        running = values[row]
        for col in range(row + 1, 6):
            running = running - entries[row][col] * result[col]
        result[row] = running / entries[row][row]
    return result


def cross(u, v):
    return [u[1] * v[2] - u[2] * v[1], u[2] * v[0] - u[0] * v[2], u[0] * v[1] - u[1] * v[0]]


def turn(at):
    return (2 + 3 * at + 3 * ((at * (at - 1)) // 2)) % 4


def kernel(
    dest_hbm, scan_hbm, src_hbm, mat_hbm, tp_hbm, tn_hbm, out_ref,
    dest_v, scan_s, src_v, mat_v, tp_v, tn_v, inv_v, inv_s, table, rhs, held,
    send, relay, recv, ucat, sums, ret_send, ret_recv, total, total_far,
    in_sem, inv_sem, send_sem, relay_sem, onward_sem, recv_sem,
    ret_ssem, ret_rsem, far_ssem, far_rsem,
):
    me_grp, me = lax.axis_index("grp"), lax.axis_index("tile")
    z, y, x = me // PLANE, (me // 4) % 4, me % 4
    level = me - me % PLANE
    spot = me % PLANE

    def in_plane(group, sign):
        dx, dy = turn(group % 4), turn(group // 4)
        return level + ((y + 4 + sign * dy) % 4) * 4 + (x + 4 + sign * dx) % 4

    def along_z(dz):
        return ((z + dz) % 8) * PLANE + spot

    copies = [
        pltpu.make_async_copy(s, d, in_sem.at[i])
        for i, (s, d) in enumerate(
            [(dest_hbm, dest_v), (scan_hbm, scan_s), (src_hbm, src_v), (mat_hbm, mat_v), (tp_hbm, tp_v), (tn_hbm, tn_v)]
        )
    ]
    for copy in copies:
        copy.start()

    barrier = pltpu.get_barrier_semaphore()
    for dz in DZ_ORDER[:-1]:
        pl.semaphore_signal(barrier, 1, device_id={"tile": along_z(dz)})

    def announce(group, carry):
        pl.semaphore_signal(barrier, 1, device_id={"tile": in_plane(group, 1)})
        return carry

    lax.fori_loop(0, 15, announce, 0, unroll=5)
    pl.semaphore_signal(barrier, 1, device_id={"grp": 1 - me_grp})

    copies[0].wait()
    blocks = jnp.broadcast_to(dest_v[...], (LANES, LANES)).T
    lane = lax.broadcasted_iota(I32, (LANES, LANES), 1)
    number = lax.broadcasted_iota(I32, (LANES, LANES), 0)
    named = blocks == lane
    first = jnp.min(jnp.where(named, number, 1000), axis=0, keepdims=True)
    last = jnp.max(jnp.where(named, number, -1), axis=0, keepdims=True)
    first = jnp.where(last < 0, -1, first)
    last = jnp.where(last == first, -1, last)
    inv_v[...] = jnp.concatenate([first, last], axis=0)
    to_smem = pltpu.make_async_copy(inv_v, inv_s, inv_sem)
    to_smem.start()
    for copy in copies[1:4]:
        copy.wait()
    to_smem.wait()

    def pack(group, carry):
        place = in_plane(group, 1) % PLANE
        for j, dz in enumerate(DZ_ORDER):
            d = ((z + dz) % 8) * PLANE + place
            slots = send.at[pl.ds(pl.multiple_of(group * LANES, LANES) + j * 16, 16)]
            for r in range(2):
                l = inv_s[r, d]
                block = jnp.minimum(jnp.maximum(l, 0), TILES - 1)
                scale = jnp.where(l >= 0, 1, 0)
                base = jnp.where(l >= 0, scan_s[0, block] * TARGET_PTS, -1)
                for c in range(3):
                    slots[r * 8 + 2 * c : r * 8 + 2 * c + 2, :] = src_v[c * TILES + block]
                slots[r * 8 + 6 : r * 8 + 8, :] = (mat_v[block] * scale + base).astype(F32)
        return carry

    lax.fori_loop(0, LEAD, pack, 0, unroll=2)
    pl.semaphore_wait(barrier, 7 + 15 + 1)

    def rows_of(group, j=0, count=8):
        return pl.ds(pl.multiple_of(group * LANES, LANES) + j * 16, count * 16)

    def z_copy(source, target, group, j, sent, sem):
        return pltpu.make_async_remote_copy(
            src_ref=source.at[rows_of(group, j, 1)],
            dst_ref=target.at[rows_of(group, j, 1)],
            send_sem=sent,
            recv_sem=sem.at[group],
            device_id={"tile": along_z(DZ_ORDER[j])},
        )

    def plane_copy(source, target, group, sent, sem):
        return pltpu.make_async_remote_copy(
            src_ref=source.at[rows_of(group)],
            dst_ref=target.at[rows_of(group)],
            send_sem=sent,
            recv_sem=sem.at[group],
            device_id={"tile": in_plane(group, 1)},
        )

    def landed(ref, group, sem, count=8):
        piece = ref.at[rows_of(group, 0, count)]
        return pltpu.make_async_copy(piece, piece, sem.at[group])

    def issue(group, carry):
        for j in range(7):
            z_copy(send, relay, group, j, send_sem, relay_sem).start()
        relay[rows_of(group, 7, 1), :] = send[rows_of(group, 7, 1), :]
        return carry

    def issue_plane(group, carry):
        plane_copy(send, relay, group, send_sem, relay_sem).start()
        return carry

    lax.fori_loop(0, LEAD, issue, 0)
    lax.fori_loop(8, 16, pack, 0, unroll=2)
    lax.fori_loop(8, 15, issue_plane, 0)
    lax.fori_loop(LEAD, 8, pack, 0, unroll=2)

    copies[4].wait()
    copies[5].wait()

    def spread(at, carry):
        rows = table.at[pl.ds(pl.multiple_of(at * 8, 8), 8)]
        columns = pl.ds(pl.multiple_of(at * LANES, LANES), LANES)
        rows[0:3, :] = tp_v[:, columns]
        rows[3:6, :] = tn_v[:, columns]
        return carry

    lax.fori_loop(0, 4 * SCANS_DEV, spread, 0, unroll=8)
    for c in range(6):
        for chunk in range(4):
            column = jnp.concatenate(
                [table[pl.ds((s8 * 32 + chunk) * 8 + c, 8, stride=32), :] for s8 in range(8)], axis=0
            )
            at = (c * 4 + chunk) * LANES
            for part, piece in enumerate(parts_of(column)):
                rhs[part * 64 : (part + 1) * 64, at : at + LANES] = piece

    lane8 = lax.broadcasted_iota(I32, (8, LANES), 1)

    def settle(groups):
        batches = [(g, r) for g in range(len(groups)) for r in range(2)]

        def rows(g, r, row):
            return recv[pl.ds(groups[g] * LANES + r * 8 + row, 8, stride=16), :]

        wanted = {(g, r, h): rows(g, r, 6 + h).astype(I32) for g, r in batches for h in range(2)}
        scan = {(g, r): lax.shift_right_arithmetic(wanted[g, r, 0][:, 0:1], 9) for g, r in batches}
        column = lax.broadcasted_iota(I32, (8, 3 * SCANS_DEV), 1) & (SCANS_DEV - 1)
        picks = jnp.concatenate([jnp.where(column == scan[b], 1.0, 0.0) for b in batches], axis=0)
        held[: picks.shape[0], :] = jnp.dot(picks.astype(jnp.bfloat16), rhs[...], preferred_element_type=F32)
        for g in range(len(groups)):
            result = jnp.zeros((8, LANES), F32)
            for r in range(2):
                terms = []
                for h in range(2):
                    inside = wanted[g, r, h] & (LANES - 1)
                    odd = (wanted[g, r, h] & LANES) != 0
                    upper = (wanted[g, r, h] & (2 * LANES)) != 0
                    found = []
                    for c in range(6):
                        got = [
                            jnp.take_along_axis(
                                held[(2 * g + r) * 8 : (2 * g + r) * 8 + 8, (4 * c + q) * LANES : (4 * c + q + 1) * LANES],
                                inside, axis=1, mode="promise_in_bounds",
                            )
                            for q in range(4)
                        ]
                        found.append(jnp.where(upper, jnp.where(odd, got[3], got[2]), jnp.where(odd, got[1], got[0])))
                    p, q, n = [rows(g, r, 2 * c + h) for c in range(3)], found[:3], found[3:]
                    a, b = cross(p, n), cross(q, n)
                    m = n[0] * (p[0] - q[0]) + n[1] * (p[1] - q[1]) + n[2] * (p[2] - q[2])
                    terms.append((a, b, n, [m]))

                def put(result, at, left, i, right, j, sign=1):
                    total = terms[0][left][i] * terms[0][right][j] + terms[1][left][i] * terms[1][right][j]
                    value = jnp.sum(total, axis=1, keepdims=True)
                    return jnp.where(lane8 == at + 64 * r, value if sign > 0 else -value, result)

                for at, (i, j) in enumerate(PAIRS):
                    result = put(result, at, 0, i, 0, j)
                    result = put(result, AT_NN + at, 2, i, 2, j)
                    result = put(result, AT_B + at, 1, i, 1, j)
                for i in range(3):
                    for j in range(3):
                        result = put(result, AT_AN + 3 * i + j, 0, i, 2, j)
                        result = put(result, AT_B + AT_AN + 3 * i + j, 1, i, 2, j)
                    result = put(result, AT_AM + i, 0, i, 3, 0)
                    result = put(result, AT_NM + i, 2, i, 3, 0)
                    result = put(result, AT_B + AT_AM + i, 1, i, 3, 0, -1)
            which = jnp.where(lane8 < 64, scan[g, 0], scan[g, 1])
            block = pl.ds(pl.multiple_of(groups[g] * 8, 8), 8)
            ucat[block, :] = jnp.where((lane8 & 63) == which, 1.0, 0.0)
            sums[block, :] = result
            for i in range(8):
                ret_send[groups[g] * 8 + i] = result[i : i + 1, :]

    def back_copy(group, j):
        to = ((z + 8 - DZ_ORDER[j]) % 8) * PLANE + in_plane(group, -1) % PLANE
        return pltpu.make_async_remote_copy(
            src_ref=ret_send.at[group * 8 + j],
            dst_ref=ret_recv.at[me],
            send_sem=ret_ssem,
            recv_sem=ret_rsem,
            device_id={"tile": to},
        )

    def give_back(group, count=8):
        for j in range(count):
            back_copy(group, j).start()

    def onward(step):
        landed(relay, step, relay_sem, 7).wait()
        plane_copy(relay, recv, step, onward_sem, recv_sem).start()

    def onward_z(group):
        landed(relay, group, relay_sem).wait()
        for j in range(7):
            z_copy(relay, recv, group, j, onward_sem, recv_sem).start()
        recv[rows_of(group, 7, 1), :] = relay[rows_of(group, 7, 1), :]

    def work(pair):
        landed(recv, pair, recv_sem).wait()
        landed(recv, pair + 8, recv_sem, 7).wait()
        settle([pair, pair + 8])
        give_back(pair)
        give_back(pair + 8)

    def early(step, carry):
        onward(step)
        onward_z(step + 8)

        @pl.when(step + LEAD < 8)
        def _():
            issue(step + LEAD, 0)

        return carry

    def early_and_work(step, carry):
        early(step, carry)
        work(step - LAG)
        return carry

    def late(pair, carry):
        work(pair)
        return carry

    lax.fori_loop(0, LAG, early, 0)
    lax.fori_loop(LAG, 7, early_and_work, 0)
    onward(7)
    for j in range(7):
        z_copy(send, recv, 15, j, send_sem, recv_sem).start()
    recv[rows_of(15, 7, 1), :] = send[rows_of(15, 7, 1), :]
    lax.fori_loop(7 - LAG, 6, late, 0)
    landed(recv, 7, recv_sem).wait()
    settle([7])
    give_back(7)
    lax.fori_loop(6, 7, late, 0)
    landed(recv, 15, recv_sem, 7).wait()
    settle([15])
    give_back(15, 7)
    ret_recv[me] = ret_send[15 * 8 + 7]

    by_target = jnp.dot(ucat[...].T, sums[...], precision=PRECISE, preferred_element_type=F32)
    by_target = by_target[:64] + pltpu.roll(by_target[64:], 64, axis=1)
    lane64 = lax.broadcasted_iota(I32, (SCANS_DEV, LANES), 1)
    moved = pltpu.roll(by_target, LANES - AT_B, axis=1)
    by_target = jnp.where(
        lane64 < AT_NN, moved, jnp.where(lane64 < AT_NM, by_target, jnp.where(lane64 < AT_NM + 3, -by_target, 0.0))
    )
    scan_row = lax.broadcasted_iota(I32, (SCANS_DEV, LANES), 0)
    owner = [lax.shift_right_arithmetic(inv_v[r : r + 1, :], 1) for r in range(2)]
    scat = jnp.concatenate([jnp.where(scan_row == owner[r], 1.0, 0.0) for r in range(2)], axis=0)

    sent = send.at[pl.ds(0, 8 * 7 * 16 + 7 * 8 * 16 + 7 * 16)]
    pltpu.make_async_copy(sent, sent, send_sem).wait()
    moved_on = relay.at[pl.ds(0, 8 * 8 * 16 + 7 * 7 * 16)]
    pltpu.make_async_copy(moved_on, moved_on, onward_sem).wait()
    others = ret_recv.at[pl.ds(0, TILES - 1)]
    pltpu.make_async_copy(others, others, ret_rsem).wait()
    gone = ret_send.at[pl.ds(0, TILES - 1)]
    pltpu.make_async_copy(gone, gone, ret_ssem).wait()
    returned = ret_recv[...].reshape(TILES, LANES)
    by_source = jnp.dot(scat, returned, precision=PRECISE, preferred_element_type=F32)
    by_source = by_source[:64] + pltpu.roll(by_source[64:], 64, axis=1)
    both = by_source + by_target
    flipped = jnp.concatenate([both, jnp.zeros_like(both)], axis=0).T
    total[...] = flipped[:32, :]
    far = pltpu.make_async_remote_copy(
        src_ref=total, dst_ref=total_far, send_sem=far_ssem, recv_sem=far_rsem, device_id={"grp": 1 - me_grp}
    )
    far.start()
    far.wait_recv()
    whole = total[...] + total_far[...]
    result = solve_rows([whole[at : at + 1, :] for at in range(27)])
    for row in range(6):
        out_ref[row : row + 1, :] = result[row]
    far.wait_send()


def body(source_points, intersection, target_scan, matches, target_points, target_normals):
    anywhere = pl.BlockSpec(memory_space=pl.ANY)
    vmem = pltpu.VMEM
    dma = pltpu.SemaphoreType.DMA
    steps = pl.pallas_call(
        kernel,
        name="icp_step",
        out_shape=jax.ShapeDtypeStruct((8, LANES), F32),
        in_specs=[anywhere] * 6,
        out_specs=pl.BlockSpec(memory_space=pltpu.VMEM),
        scratch_shapes=[
            vmem((1, TILES), I32),
            pltpu.SMEM((1, TILES), I32),
            vmem((3 * TILES, 2, LANES), F32),
            vmem((TILES, 2, LANES), I32),
            vmem((3, SCANS_DEV * TARGET_PTS), F32),
            vmem((3, SCANS_DEV * TARGET_PTS), F32),
            vmem((2, TILES), I32),
            pltpu.SMEM((2, TILES), I32),
            vmem((SCANS_DEV * 4 * 8 + 32, LANES), F32),
            vmem((3 * SCANS_DEV, 6 * TARGET_PTS), jnp.bfloat16),
            vmem((32, 6 * TARGET_PTS), F32),
            vmem((TILES * 16, LANES), F32),
            vmem((TILES * 16, LANES), F32),
            vmem((TILES * 16 + 16, LANES), F32),
            vmem((TILES, LANES), F32),
            vmem((TILES, LANES), F32),
            vmem((TILES, 1, LANES), F32),
            vmem((TILES, 1, LANES), F32),
            vmem((32, LANES), F32),
            vmem((32, LANES), F32),
            dma((6,)),
            dma,
            dma,
            dma((16,)),
            dma,
            dma((16,)),
            dma,
            dma,
            dma,
            dma,
        ],
        compiler_params=pltpu.CompilerParams(collective_id=0, has_side_effects=True),
    )(
        intersection.reshape(1, TILES),
        target_scan,
        source_points.reshape(3 * TILES, 2, LANES),
        matches.reshape(TILES, 2, LANES),
        target_points,
        target_normals,
    )
    return steps[:6, :SCANS_DEV]


def solution(mesh):
    in_specs = (
        P("grp", None, "tile"),
        P("grp", "tile", None),
        P("grp", "tile"),
        P("grp", "tile"),
        P(None, "tile"),
        P(None, "tile"),
    )
    return jax.shard_map(body, mesh=mesh, in_specs=in_specs, out_specs=P(None, "tile"), check_vma=False)
```

```python
import jax
import jax.numpy as jnp
from jax import lax
from jax.experimental import pallas as pl
from jax.experimental.pallas import tpu as pltpu
from jax.sharding import PartitionSpec as P

TILES = 128
SCANS_DEV = 64
TARGET_PTS = 512
LANES = 128
DAMPING = 0.1
PRECISE = lax.Precision.HIGHEST
F32 = jnp.float32
I32 = jnp.int32
DZ_ORDER = (4, 3, 5, 2, 6, 1, 7, 0)
PLANE = 16

PAIRS = [(i, j) for i in range(3) for j in range(i, 3)]
AT_AN, AT_AM, AT_NN, AT_NM, AT_B = 6, 15, 18, 24, 32


def parts_of(value):
    high = value.astype(jnp.bfloat16)
    rest = value - high.astype(F32)
    middle = rest.astype(jnp.bfloat16)
    low = (rest - middle.astype(F32)).astype(jnp.bfloat16)
    return high, middle, low


def solve_rows(rows):
    entries = [[None] * 6 for _ in range(6)]
    for at, (i, j) in enumerate(PAIRS):
        entries[i][j] = entries[j][i] = rows[at]
        entries[3 + i][3 + j] = entries[3 + j][3 + i] = rows[AT_NN + at]
    for i in range(3):
        for j in range(3):
            entries[i][3 + j] = entries[3 + j][i] = rows[AT_AN + 3 * i + j]
    traced = entries[0][0]
    for at in range(1, 6):
        traced = traced + entries[at][at]
    shift_by = DAMPING * traced / 6.0
    for at in range(6):
        entries[at][at] = entries[at][at] + shift_by
    values = [-rows[AT_AM + i] for i in range(3)] + [-rows[AT_NM + i] for i in range(3)]
    for pivot in range(6):
        for row in range(pivot + 1, 6):
            factor = entries[row][pivot] / entries[pivot][pivot]
            for col in range(pivot + 1, 6):
                entries[row][col] = entries[row][col] - factor * entries[pivot][col]
            values[row] = values[row] - factor * values[pivot]
    result = [None] * 6
    for row in range(5, -1, -1):
        running = values[row]
        for col in range(row + 1, 6):
            running = running - entries[row][col] * result[col]
        result[row] = running / entries[row][row]
    return result


def cross(u, v):
    return [u[1] * v[2] - u[2] * v[1], u[2] * v[0] - u[0] * v[2], u[0] * v[1] - u[1] * v[0]]


def turn(at):
    return (2 + 3 * at + 3 * ((at * (at - 1)) // 2)) % 4


def kernel(
    dest_hbm, scan_hbm, src_hbm, mat_hbm, tp_hbm, tn_hbm, out_ref,
    dest_v, scan_s, src_v, mat_v, tp_v, tn_v, inv_v, inv_s, table, rhs, held,
    send, relay, recv, ucat, sums, ret_send, ret_recv, total, total_far,
    ready_sem, in_sem, inv_sem, send_sem, relay_sem, onward_sem, recv_sem,
    ret_ssem, ret_rsem, far_ssem, far_rsem,
):
    me_grp, me = lax.axis_index("grp"), lax.axis_index("tile")
    z, y, x = me // PLANE, (me // 4) % 4, me % 4
    level = me - me % PLANE
    spot = me % PLANE

    def in_plane(group, sign):
        half = group // 8
        dx = turn((1 - half) * (group // 2) + half * (group % 4))
        dy = (1 - half) * (2 + group % 2) + half * (3 - group // 4)
        return level + ((y + 4 + sign * dy) % 4) * 4 + (x + 4 + sign * dx) % 4

    def along_z(dz):
        return ((z + dz) % 8) * PLANE + spot

    x_peers = [level + y * 4 + (x + at) % 4 for at in (2, 1, 3)]
    y_peers = [level + ((y + at) % 4) * 4 + x for at in (2, 1, 3)]
    barrier = pltpu.get_barrier_semaphore()
    for peer in [along_z(dz) for dz in DZ_ORDER[:-1]] + y_peers + x_peers:
        pl.semaphore_signal(barrier, 1, device_id={"tile": peer})
    pl.semaphore_signal(barrier, 1, device_id={"grp": 1 - me_grp})

    copies = [
        pltpu.make_async_copy(s, d, in_sem.at[i])
        for i, (s, d) in enumerate(
            [(dest_hbm, dest_v), (scan_hbm, scan_s), (src_hbm, src_v), (mat_hbm, mat_v), (tp_hbm, tp_v), (tn_hbm, tn_v)]
        )
    ]
    for copy in copies:
        copy.start()

    copies[0].wait()
    blocks = jnp.broadcast_to(dest_v[...], (LANES, LANES)).T
    lane = lax.broadcasted_iota(I32, (LANES, LANES), 1)
    number = lax.broadcasted_iota(I32, (LANES, LANES), 0)
    named = blocks == lane
    first = jnp.min(jnp.where(named, number, 1000), axis=0, keepdims=True)
    last = jnp.max(jnp.where(named, number, -1), axis=0, keepdims=True)
    first = jnp.where(last < 0, -1, first)
    last = jnp.where(last == first, -1, last)
    inv_v[...] = jnp.concatenate([first, last], axis=0)
    to_smem = pltpu.make_async_copy(inv_v, inv_s, inv_sem)
    to_smem.start()
    for copy in copies[1:4]:
        copy.wait()
    to_smem.wait()

    def pack(group, carry):
        place = in_plane(group, 1) % PLANE
        for j, dz in enumerate(DZ_ORDER):
            d = ((z + dz) % 8) * PLANE + place
            slots = send.at[pl.ds(pl.multiple_of(group * LANES, LANES) + j * 16, 16)]
            for r in range(2):
                l = inv_s[r, d]
                block = jnp.minimum(jnp.maximum(l, 0), TILES - 1)
                scale = jnp.where(l >= 0, 1, 0)
                base = jnp.where(l >= 0, scan_s[0, block] * TARGET_PTS, -1)
                for c in range(3):
                    slots[r * 8 + 2 * c : r * 8 + 2 * c + 2, :] = src_v[c * TILES + block]
                slots[r * 8 + 6 : r * 8 + 8, :] = (mat_v[block] * scale + base).astype(F32)
        return carry

    lax.fori_loop(0, 8, pack, 0, unroll=2)
    pl.semaphore_wait(barrier, 7 + 3 + 3 + 1)
    for peer in x_peers:
        pl.semaphore_signal(ready_sem, 1, device_id={"tile": peer})

    def rows_of(group, j=0, count=8):
        return pl.ds(pl.multiple_of(group * LANES, LANES) + j * 16, count * 16)

    def z_copy(source, target, group, j, sent, sem):
        return pltpu.make_async_remote_copy(
            src_ref=source.at[rows_of(group, j, 1)],
            dst_ref=target.at[rows_of(group, j, 1)],
            send_sem=sent,
            recv_sem=sem.at[group],
            device_id={"tile": along_z(DZ_ORDER[j])},
        )

    def plane_copy(source, target, group, sent, sem):
        return pltpu.make_async_remote_copy(
            src_ref=source.at[rows_of(group)],
            dst_ref=target.at[rows_of(group)],
            send_sem=sent,
            recv_sem=sem.at[group],
            device_id={"tile": in_plane(group, 1)},
        )

    def landed(ref, group, sem, count=8):
        piece = ref.at[rows_of(group, 0, count)]
        return pltpu.make_async_copy(piece, piece, sem.at[group])

    def issue(group, carry):
        for j in range(7):
            z_copy(send, relay, group, j, send_sem, relay_sem).start()
        relay[rows_of(group, 7, 1), :] = send[rows_of(group, 7, 1), :]
        return carry

    def issue_plane(group, carry):
        plane_copy(send, relay, group, send_sem, relay_sem).start()
        return carry

    lax.fori_loop(0, 8, issue, 0)
    lax.fori_loop(8, 16, pack, 0, unroll=2)
    pl.semaphore_wait(ready_sem, 3)
    lax.fori_loop(8, 15, issue_plane, 0)

    copies[4].wait()
    copies[5].wait()

    def spread(at, carry):
        rows = table.at[pl.ds(pl.multiple_of(at * 8, 8), 8)]
        columns = pl.ds(pl.multiple_of(at * LANES, LANES), LANES)
        rows[0:3, :] = tp_v[:, columns]
        rows[3:6, :] = tn_v[:, columns]
        return carry

    lax.fori_loop(0, 4 * SCANS_DEV, spread, 0, unroll=8)
    for c in range(6):
        for chunk in range(4):
            column = jnp.concatenate(
                [table[pl.ds((s8 * 32 + chunk) * 8 + c, 8, stride=32), :] for s8 in range(8)], axis=0
            )
            at = (c * 4 + chunk) * LANES
            for part, piece in enumerate(parts_of(column)):
                rhs[part * 64 : (part + 1) * 64, at : at + LANES] = piece

    lane8 = lax.broadcasted_iota(I32, (8, LANES), 1)

    def settle(groups):
        batches = [(g, r) for g in range(len(groups)) for r in range(2)]

        def rows(g, r, row):
            return recv[pl.ds(groups[g] * LANES + r * 8 + row, 8, stride=16), :]

        wanted = {(g, r, h): rows(g, r, 6 + h).astype(I32) for g, r in batches for h in range(2)}
        scan = {(g, r): lax.shift_right_arithmetic(wanted[g, r, 0][:, 0:1], 9) for g, r in batches}
        column = lax.broadcasted_iota(I32, (8, 3 * SCANS_DEV), 1) & (SCANS_DEV - 1)
        picks = jnp.concatenate([jnp.where(column == scan[b], 1.0, 0.0) for b in batches], axis=0)
        held[: picks.shape[0], :] = jnp.dot(picks.astype(jnp.bfloat16), rhs[...], preferred_element_type=F32)
        for g in range(len(groups)):
            result = jnp.zeros((8, LANES), F32)
            for r in range(2):
                terms = []
                for h in range(2):
                    inside = wanted[g, r, h] & (LANES - 1)
                    odd = (wanted[g, r, h] & LANES) != 0
                    upper = (wanted[g, r, h] & (2 * LANES)) != 0
                    found = []
                    for c in range(6):
                        got = [
                            jnp.take_along_axis(
                                held[(2 * g + r) * 8 : (2 * g + r) * 8 + 8, (4 * c + q) * LANES : (4 * c + q + 1) * LANES],
                                inside, axis=1, mode="promise_in_bounds",
                            )
                            for q in range(4)
                        ]
                        found.append(jnp.where(upper, jnp.where(odd, got[3], got[2]), jnp.where(odd, got[1], got[0])))
                    p, q, n = [rows(g, r, 2 * c + h) for c in range(3)], found[:3], found[3:]
                    a, b = cross(p, n), cross(q, n)
                    m = n[0] * (p[0] - q[0]) + n[1] * (p[1] - q[1]) + n[2] * (p[2] - q[2])
                    terms.append((a, b, n, [m]))

                def put(result, at, left, i, right, j, sign=1):
                    total = terms[0][left][i] * terms[0][right][j] + terms[1][left][i] * terms[1][right][j]
                    value = jnp.sum(total, axis=1, keepdims=True)
                    return jnp.where(lane8 == at + 64 * r, value if sign > 0 else -value, result)

                for at, (i, j) in enumerate(PAIRS):
                    result = put(result, at, 0, i, 0, j)
                    result = put(result, AT_NN + at, 2, i, 2, j)
                    result = put(result, AT_B + at, 1, i, 1, j)
                for i in range(3):
                    for j in range(3):
                        result = put(result, AT_AN + 3 * i + j, 0, i, 2, j)
                        result = put(result, AT_B + AT_AN + 3 * i + j, 1, i, 2, j)
                    result = put(result, AT_AM + i, 0, i, 3, 0)
                    result = put(result, AT_NM + i, 2, i, 3, 0)
                    result = put(result, AT_B + AT_AM + i, 1, i, 3, 0, -1)
            which = jnp.where(lane8 < 64, scan[g, 0], scan[g, 1])
            block = pl.ds(pl.multiple_of(groups[g] * 8, 8), 8)
            ucat[block, :] = jnp.where((lane8 & 63) == which, 1.0, 0.0)
            sums[block, :] = result
            for i in range(8):
                ret_send[groups[g] * 8 + i] = result[i : i + 1, :]

    def back_copy(group, j):
        to = ((z + 8 - DZ_ORDER[j]) % 8) * PLANE + in_plane(group, -1) % PLANE
        return pltpu.make_async_remote_copy(
            src_ref=ret_send.at[group * 8 + j],
            dst_ref=ret_recv.at[me],
            send_sem=ret_ssem,
            recv_sem=ret_rsem,
            device_id={"tile": to},
        )

    def give_back(group, count=8):
        for j in range(count):
            back_copy(group, j).start()

    def onward(step):
        landed(relay, step, relay_sem, 7).wait()
        plane_copy(relay, recv, step, onward_sem, recv_sem).start()

    def onward_z(group):
        landed(relay, group, relay_sem).wait()
        for j in range(7):
            z_copy(relay, recv, group, j, onward_sem, recv_sem).start()
        recv[rows_of(group, 7, 1), :] = relay[rows_of(group, 7, 1), :]

    def early(step, carry):
        onward(step)
        onward_z(step + 8)
        return carry

    def late(step, carry):
        landed(recv, step + 1, recv_sem).wait()
        landed(recv, step + 8, recv_sem, 7).wait()
        settle([step + 1, step + 8])
        give_back(step + 1)
        give_back(step + 8)
        return carry

    lax.fori_loop(0, 7, early, 0)
    onward(7)
    for j in range(7):
        z_copy(send, recv, 15, j, send_sem, recv_sem).start()
    recv[rows_of(15, 7, 1), :] = send[rows_of(15, 7, 1), :]
    landed(recv, 0, recv_sem).wait()
    settle([0])
    give_back(0)
    lax.fori_loop(0, 7, late, 0)
    landed(recv, 15, recv_sem, 7).wait()
    settle([15])
    give_back(15, 7)
    ret_recv[me] = ret_send[15 * 8 + 7]

    by_target = jnp.dot(ucat[...].T, sums[...], precision=PRECISE, preferred_element_type=F32)
    by_target = by_target[:64] + pltpu.roll(by_target[64:], 64, axis=1)
    lane64 = lax.broadcasted_iota(I32, (SCANS_DEV, LANES), 1)
    moved = pltpu.roll(by_target, LANES - AT_B, axis=1)
    by_target = jnp.where(
        lane64 < AT_NN, moved, jnp.where(lane64 < AT_NM, by_target, jnp.where(lane64 < AT_NM + 3, -by_target, 0.0))
    )
    scan_row = lax.broadcasted_iota(I32, (SCANS_DEV, LANES), 0)
    owner = [lax.shift_right_arithmetic(inv_v[r : r + 1, :], 1) for r in range(2)]
    scat = jnp.concatenate([jnp.where(scan_row == owner[r], 1.0, 0.0) for r in range(2)], axis=0)

    sent = send.at[pl.ds(0, 8 * 7 * 16 + 7 * 8 * 16 + 7 * 16)]
    pltpu.make_async_copy(sent, sent, send_sem).wait()
    moved_on = relay.at[pl.ds(0, 8 * 8 * 16 + 7 * 7 * 16)]
    pltpu.make_async_copy(moved_on, moved_on, onward_sem).wait()
    others = ret_recv.at[pl.ds(0, TILES - 1)]
    pltpu.make_async_copy(others, others, ret_rsem).wait()
    gone = ret_send.at[pl.ds(0, TILES - 1)]
    pltpu.make_async_copy(gone, gone, ret_ssem).wait()
    returned = ret_recv[...].reshape(TILES, LANES)
    by_source = jnp.dot(scat, returned, precision=PRECISE, preferred_element_type=F32)
    by_source = by_source[:64] + pltpu.roll(by_source[64:], 64, axis=1)
    both = by_source + by_target
    flipped = jnp.concatenate([both, jnp.zeros_like(both)], axis=0).T
    total[...] = flipped[:32, :]
    far = pltpu.make_async_remote_copy(
        src_ref=total, dst_ref=total_far, send_sem=far_ssem, recv_sem=far_rsem, device_id={"grp": 1 - me_grp}
    )
    far.start()
    far.wait_recv()
    whole = total[...] + total_far[...]
    result = solve_rows([whole[at : at + 1, :] for at in range(27)])
    for row in range(6):
        out_ref[row : row + 1, :] = result[row]
    far.wait_send()


def body(source_points, intersection, target_scan, matches, target_points, target_normals):
    anywhere = pl.BlockSpec(memory_space=pl.ANY)
    vmem = pltpu.VMEM
    dma = pltpu.SemaphoreType.DMA
    steps = pl.pallas_call(
        kernel,
        name="icp_step",
        out_shape=jax.ShapeDtypeStruct((8, LANES), F32),
        in_specs=[anywhere] * 6,
        out_specs=pl.BlockSpec(memory_space=pltpu.VMEM),
        scratch_shapes=[
            vmem((1, TILES), I32),
            pltpu.SMEM((1, TILES), I32),
            vmem((3 * TILES, 2, LANES), F32),
            vmem((TILES, 2, LANES), I32),
            vmem((3, SCANS_DEV * TARGET_PTS), F32),
            vmem((3, SCANS_DEV * TARGET_PTS), F32),
            vmem((2, TILES), I32),
            pltpu.SMEM((2, TILES), I32),
            vmem((SCANS_DEV * 4 * 8 + 32, LANES), F32),
            vmem((3 * SCANS_DEV, 6 * TARGET_PTS), jnp.bfloat16),
            vmem((32, 6 * TARGET_PTS), F32),
            vmem((TILES * 16, LANES), F32),
            vmem((TILES * 16, LANES), F32),
            vmem((TILES * 16 + 16, LANES), F32),
            vmem((TILES, LANES), F32),
            vmem((TILES, LANES), F32),
            vmem((TILES, 1, LANES), F32),
            vmem((TILES, 1, LANES), F32),
            vmem((32, LANES), F32),
            vmem((32, LANES), F32),
            pltpu.SemaphoreType.REGULAR,
            dma((6,)),
            dma,
            dma,
            dma((16,)),
            dma,
            dma((16,)),
            dma,
            dma,
            dma,
            dma,
        ],
        compiler_params=pltpu.CompilerParams(collective_id=0, has_side_effects=True),
    )(
        intersection.reshape(1, TILES),
        target_scan,
        source_points.reshape(3 * TILES, 2, LANES),
        matches.reshape(TILES, 2, LANES),
        target_points,
        target_normals,
    )
    return steps[:6, :SCANS_DEV]


def solution(mesh):
    in_specs = (
        P("grp", None, "tile"),
        P("grp", "tile", None),
        P("grp", "tile"),
        P("grp", "tile"),
        P(None, "tile"),
        P(None, "tile"),
    )
    return jax.shard_map(body, mesh=mesh, in_specs=in_specs, out_specs=P(None, "tile"), check_vma=False)
```

```python
import jax
import jax.numpy as jnp
from jax import lax
from jax.experimental import pallas as pl
from jax.experimental.pallas import tpu as pltpu
from jax.sharding import PartitionSpec as P

TILES = 128
SCANS_DEV = 64
TARGET_PTS = 512
LANES = 128
DAMPING = 0.1
PRECISE = lax.Precision.HIGHEST
F32 = jnp.float32
I32 = jnp.int32
DZ_ORDER = (4, 3, 5, 2, 6, 1, 7, 0)
PLANE = 16

PAIRS = [(i, j) for i in range(3) for j in range(i, 3)]
AT_AN, AT_AM, AT_NN, AT_NM, AT_B = 6, 15, 18, 24, 32


def parts_of(value):
    high = value.astype(jnp.bfloat16)
    rest = value - high.astype(F32)
    middle = rest.astype(jnp.bfloat16)
    low = (rest - middle.astype(F32)).astype(jnp.bfloat16)
    return high, middle, low


def solve_rows(rows):
    entries = [[None] * 6 for _ in range(6)]
    for at, (i, j) in enumerate(PAIRS):
        entries[i][j] = entries[j][i] = rows[at]
        entries[3 + i][3 + j] = entries[3 + j][3 + i] = rows[AT_NN + at]
    for i in range(3):
        for j in range(3):
            entries[i][3 + j] = entries[3 + j][i] = rows[AT_AN + 3 * i + j]
    traced = entries[0][0]
    for at in range(1, 6):
        traced = traced + entries[at][at]
    shift_by = DAMPING * traced / 6.0
    for at in range(6):
        entries[at][at] = entries[at][at] + shift_by
    values = [-rows[AT_AM + i] for i in range(3)] + [-rows[AT_NM + i] for i in range(3)]
    for pivot in range(6):
        for row in range(pivot + 1, 6):
            factor = entries[row][pivot] / entries[pivot][pivot]
            for col in range(pivot + 1, 6):
                entries[row][col] = entries[row][col] - factor * entries[pivot][col]
            values[row] = values[row] - factor * values[pivot]
    result = [None] * 6
    for row in range(5, -1, -1):
        running = values[row]
        for col in range(row + 1, 6):
            running = running - entries[row][col] * result[col]
        result[row] = running / entries[row][row]
    return result


def cross(u, v):
    return [u[1] * v[2] - u[2] * v[1], u[2] * v[0] - u[0] * v[2], u[0] * v[1] - u[1] * v[0]]


def turn(at):
    return (2 + 3 * at + 3 * ((at * (at - 1)) // 2)) % 4


def kernel(
    dest_hbm, scan_hbm, src_hbm, mat_hbm, tp_hbm, tn_hbm, out_ref,
    dest_v, scan_s, src_v, mat_v, tp_v, tn_v, inv_v, inv_s, table, rhs, held,
    send, relay, recv, ucat, sums, ret_send, ret_recv, total, total_far,
    ready_sem, in_sem, inv_sem, send_sem, relay_sem, onward_sem, recv_sem,
    ret_ssem, ret_rsem, far_ssem, far_rsem,
):
    me_grp, me = lax.axis_index("grp"), lax.axis_index("tile")
    z, y, x = me // PLANE, (me // 4) % 4, me % 4
    level = me - me % PLANE
    spot = me % PLANE

    def in_plane(group, sign):
        half = group // 8
        dx = turn((1 - half) * (group // 2) + half * (group % 4))
        dy = (1 - half) * (2 + group % 2) + half * (3 - group // 4)
        return level + ((y + 4 + sign * dy) % 4) * 4 + (x + 4 + sign * dx) % 4

    def along_z(dz):
        return ((z + dz) % 8) * PLANE + spot

    x_peers = [level + y * 4 + (x + at) % 4 for at in (2, 1, 3)]
    y_peers = [level + ((y + at) % 4) * 4 + x for at in (2, 1, 3)]
    barrier = pltpu.get_barrier_semaphore()
    for peer in [along_z(dz) for dz in DZ_ORDER[:-1]] + y_peers + x_peers:
        pl.semaphore_signal(barrier, 1, device_id={"tile": peer})
    pl.semaphore_signal(barrier, 1, device_id={"grp": 1 - me_grp})

    copies = [
        pltpu.make_async_copy(s, d, in_sem.at[i])
        for i, (s, d) in enumerate(
            [(dest_hbm, dest_v), (scan_hbm, scan_s), (src_hbm, src_v), (mat_hbm, mat_v), (tp_hbm, tp_v), (tn_hbm, tn_v)]
        )
    ]
    for copy in copies:
        copy.start()

    copies[0].wait()
    blocks = jnp.broadcast_to(dest_v[...], (LANES, LANES)).T
    lane = lax.broadcasted_iota(I32, (LANES, LANES), 1)
    number = lax.broadcasted_iota(I32, (LANES, LANES), 0)
    named = blocks == lane
    first = jnp.min(jnp.where(named, number, 1000), axis=0, keepdims=True)
    last = jnp.max(jnp.where(named, number, -1), axis=0, keepdims=True)
    first = jnp.where(last < 0, -1, first)
    last = jnp.where(last == first, -1, last)
    inv_v[...] = jnp.concatenate([first, last], axis=0)
    to_smem = pltpu.make_async_copy(inv_v, inv_s, inv_sem)
    to_smem.start()
    for copy in copies[1:4]:
        copy.wait()
    to_smem.wait()

    def pack(group, carry):
        place = in_plane(group, 1) % PLANE
        for j, dz in enumerate(DZ_ORDER):
            d = ((z + dz) % 8) * PLANE + place
            slots = send.at[pl.ds(pl.multiple_of(group * LANES, LANES) + j * 16, 16)]
            for r in range(2):
                l = inv_s[r, d]
                block = jnp.minimum(jnp.maximum(l, 0), TILES - 1)
                scale = jnp.where(l >= 0, 1, 0)
                base = jnp.where(l >= 0, scan_s[0, block] * TARGET_PTS, -1)
                for c in range(3):
                    slots[r * 8 + 2 * c : r * 8 + 2 * c + 2, :] = src_v[c * TILES + block]
                slots[r * 8 + 6 : r * 8 + 8, :] = (mat_v[block] * scale + base).astype(F32)
        return carry

    lax.fori_loop(0, 2, pack, 0, unroll=2)
    pl.semaphore_wait(barrier, 7 + 3 + 3 + 1)
    for peer in x_peers:
        pl.semaphore_signal(ready_sem, 1, device_id={"tile": peer})

    def rows_of(group, j=0, count=8):
        return pl.ds(pl.multiple_of(group * LANES, LANES) + j * 16, count * 16)

    def z_copy(source, target, group, j, sent, sem):
        return pltpu.make_async_remote_copy(
            src_ref=source.at[rows_of(group, j, 1)],
            dst_ref=target.at[rows_of(group, j, 1)],
            send_sem=sent,
            recv_sem=sem.at[group],
            device_id={"tile": along_z(DZ_ORDER[j])},
        )

    def plane_copy(source, target, group, sent, sem):
        return pltpu.make_async_remote_copy(
            src_ref=source.at[rows_of(group)],
            dst_ref=target.at[rows_of(group)],
            send_sem=sent,
            recv_sem=sem.at[group],
            device_id={"tile": in_plane(group, 1)},
        )

    def landed(ref, group, sem, count=8):
        piece = ref.at[rows_of(group, 0, count)]
        return pltpu.make_async_copy(piece, piece, sem.at[group])

    def issue(group, carry):
        for j in range(7):
            z_copy(send, relay, group, j, send_sem, relay_sem).start()
        relay[rows_of(group, 7, 1), :] = send[rows_of(group, 7, 1), :]
        return carry

    def issue_plane(group, carry):
        plane_copy(send, relay, group, send_sem, relay_sem).start()
        return carry

    def pack_and_issue(group, carry):
        pack(group, carry)
        return issue(group, carry)

    lax.fori_loop(0, 2, issue, 0)
    lax.fori_loop(2, 8, pack_and_issue, 0)
    lax.fori_loop(8, 16, pack, 0, unroll=2)
    pl.semaphore_wait(ready_sem, 3)
    lax.fori_loop(8, 15, issue_plane, 0)

    copies[4].wait()
    copies[5].wait()

    def spread(at, carry):
        rows = table.at[pl.ds(pl.multiple_of(at * 8, 8), 8)]
        columns = pl.ds(pl.multiple_of(at * LANES, LANES), LANES)
        rows[0:3, :] = tp_v[:, columns]
        rows[3:6, :] = tn_v[:, columns]
        return carry

    lax.fori_loop(0, 4 * SCANS_DEV, spread, 0, unroll=8)
    for c in range(6):
        for chunk in range(4):
            column = jnp.concatenate(
                [table[pl.ds((s8 * 32 + chunk) * 8 + c, 8, stride=32), :] for s8 in range(8)], axis=0
            )
            at = (c * 4 + chunk) * LANES
            for part, piece in enumerate(parts_of(column)):
                rhs[part * 64 : (part + 1) * 64, at : at + LANES] = piece

    lane8 = lax.broadcasted_iota(I32, (8, LANES), 1)

    def settle(groups):
        batches = [(g, r) for g in range(len(groups)) for r in range(2)]

        def rows(g, r, row):
            return recv[pl.ds(groups[g] * LANES + r * 8 + row, 8, stride=16), :]

        wanted = {(g, r, h): rows(g, r, 6 + h).astype(I32) for g, r in batches for h in range(2)}
        scan = {(g, r): lax.shift_right_arithmetic(wanted[g, r, 0][:, 0:1], 9) for g, r in batches}
        column = lax.broadcasted_iota(I32, (8, 3 * SCANS_DEV), 1) & (SCANS_DEV - 1)
        picks = jnp.concatenate([jnp.where(column == scan[b], 1.0, 0.0) for b in batches], axis=0)
        held[: picks.shape[0], :] = jnp.dot(picks.astype(jnp.bfloat16), rhs[...], preferred_element_type=F32)
        for g in range(len(groups)):
            result = jnp.zeros((8, LANES), F32)
            for r in range(2):
                terms = []
                for h in range(2):
                    inside = wanted[g, r, h] & (LANES - 1)
                    odd = (wanted[g, r, h] & LANES) != 0
                    upper = (wanted[g, r, h] & (2 * LANES)) != 0
                    found = []
                    for c in range(6):
                        got = [
                            jnp.take_along_axis(
                                held[(2 * g + r) * 8 : (2 * g + r) * 8 + 8, (4 * c + q) * LANES : (4 * c + q + 1) * LANES],
                                inside, axis=1, mode="promise_in_bounds",
                            )
                            for q in range(4)
                        ]
                        found.append(jnp.where(upper, jnp.where(odd, got[3], got[2]), jnp.where(odd, got[1], got[0])))
                    p, q, n = [rows(g, r, 2 * c + h) for c in range(3)], found[:3], found[3:]
                    a, b = cross(p, n), cross(q, n)
                    m = n[0] * (p[0] - q[0]) + n[1] * (p[1] - q[1]) + n[2] * (p[2] - q[2])
                    terms.append((a, b, n, [m]))

                def put(result, at, left, i, right, j, sign=1):
                    total = terms[0][left][i] * terms[0][right][j] + terms[1][left][i] * terms[1][right][j]
                    value = jnp.sum(total, axis=1, keepdims=True)
                    return jnp.where(lane8 == at + 64 * r, value if sign > 0 else -value, result)

                for at, (i, j) in enumerate(PAIRS):
                    result = put(result, at, 0, i, 0, j)
                    result = put(result, AT_NN + at, 2, i, 2, j)
                    result = put(result, AT_B + at, 1, i, 1, j)
                for i in range(3):
                    for j in range(3):
                        result = put(result, AT_AN + 3 * i + j, 0, i, 2, j)
                        result = put(result, AT_B + AT_AN + 3 * i + j, 1, i, 2, j)
                    result = put(result, AT_AM + i, 0, i, 3, 0)
                    result = put(result, AT_NM + i, 2, i, 3, 0)
                    result = put(result, AT_B + AT_AM + i, 1, i, 3, 0, -1)
            which = jnp.where(lane8 < 64, scan[g, 0], scan[g, 1])
            block = pl.ds(pl.multiple_of(groups[g] * 8, 8), 8)
            ucat[block, :] = jnp.where((lane8 & 63) == which, 1.0, 0.0)
            sums[block, :] = result
            for i in range(8):
                ret_send[groups[g] * 8 + i] = result[i : i + 1, :]

    def back_copy(group, j):
        to = ((z + 8 - DZ_ORDER[j]) % 8) * PLANE + in_plane(group, -1) % PLANE
        return pltpu.make_async_remote_copy(
            src_ref=ret_send.at[group * 8 + j],
            dst_ref=ret_recv.at[me],
            send_sem=ret_ssem,
            recv_sem=ret_rsem,
            device_id={"tile": to},
        )

    def give_back(group, count=8):
        for j in range(count):
            back_copy(group, j).start()

    def onward(step):
        landed(relay, step, relay_sem, 7).wait()
        plane_copy(relay, recv, step, onward_sem, recv_sem).start()

    def onward_z(group):
        landed(relay, group, relay_sem).wait()
        for j in range(7):
            z_copy(relay, recv, group, j, onward_sem, recv_sem).start()
        recv[rows_of(group, 7, 1), :] = relay[rows_of(group, 7, 1), :]

    def early(step, carry):
        onward(step)
        onward_z(step + 8)
        return carry

    def late(step, carry):
        landed(recv, step + 1, recv_sem).wait()
        landed(recv, step + 8, recv_sem, 7).wait()
        settle([step + 1, step + 8])
        give_back(step + 1)
        give_back(step + 8)
        return carry

    lax.fori_loop(0, 7, early, 0)
    onward(7)
    for j in range(7):
        z_copy(send, recv, 15, j, send_sem, recv_sem).start()
    recv[rows_of(15, 7, 1), :] = send[rows_of(15, 7, 1), :]
    landed(recv, 0, recv_sem).wait()
    settle([0])
    give_back(0)
    lax.fori_loop(0, 7, late, 0)
    landed(recv, 15, recv_sem, 7).wait()
    settle([15])
    give_back(15, 7)
    ret_recv[me] = ret_send[15 * 8 + 7]

    by_target = jnp.dot(ucat[...].T, sums[...], precision=PRECISE, preferred_element_type=F32)
    by_target = by_target[:64] + pltpu.roll(by_target[64:], 64, axis=1)
    lane64 = lax.broadcasted_iota(I32, (SCANS_DEV, LANES), 1)
    moved = pltpu.roll(by_target, LANES - AT_B, axis=1)
    by_target = jnp.where(
        lane64 < AT_NN, moved, jnp.where(lane64 < AT_NM, by_target, jnp.where(lane64 < AT_NM + 3, -by_target, 0.0))
    )
    scan_row = lax.broadcasted_iota(I32, (SCANS_DEV, LANES), 0)
    owner = [lax.shift_right_arithmetic(inv_v[r : r + 1, :], 1) for r in range(2)]
    scat = jnp.concatenate([jnp.where(scan_row == owner[r], 1.0, 0.0) for r in range(2)], axis=0)

    sent = send.at[pl.ds(0, 8 * 7 * 16 + 7 * 8 * 16 + 7 * 16)]
    pltpu.make_async_copy(sent, sent, send_sem).wait()
    moved_on = relay.at[pl.ds(0, 8 * 8 * 16 + 7 * 7 * 16)]
    pltpu.make_async_copy(moved_on, moved_on, onward_sem).wait()
    others = ret_recv.at[pl.ds(0, TILES - 1)]
    pltpu.make_async_copy(others, others, ret_rsem).wait()
    gone = ret_send.at[pl.ds(0, TILES - 1)]
    pltpu.make_async_copy(gone, gone, ret_ssem).wait()
    returned = ret_recv[...].reshape(TILES, LANES)
    by_source = jnp.dot(scat, returned, precision=PRECISE, preferred_element_type=F32)
    by_source = by_source[:64] + pltpu.roll(by_source[64:], 64, axis=1)
    both = by_source + by_target
    flipped = jnp.concatenate([both, jnp.zeros_like(both)], axis=0).T
    total[...] = flipped[:32, :]
    far = pltpu.make_async_remote_copy(
        src_ref=total, dst_ref=total_far, send_sem=far_ssem, recv_sem=far_rsem, device_id={"grp": 1 - me_grp}
    )
    far.start()
    far.wait_recv()
    whole = total[...] + total_far[...]
    result = solve_rows([whole[at : at + 1, :] for at in range(27)])
    for row in range(6):
        out_ref[row : row + 1, :] = result[row]
    far.wait_send()


def body(source_points, intersection, target_scan, matches, target_points, target_normals):
    anywhere = pl.BlockSpec(memory_space=pl.ANY)
    vmem = pltpu.VMEM
    dma = pltpu.SemaphoreType.DMA
    steps = pl.pallas_call(
        kernel,
        name="icp_step",
        out_shape=jax.ShapeDtypeStruct((8, LANES), F32),
        in_specs=[anywhere] * 6,
        out_specs=pl.BlockSpec(memory_space=pltpu.VMEM),
        scratch_shapes=[
            vmem((1, TILES), I32),
            pltpu.SMEM((1, TILES), I32),
            vmem((3 * TILES, 2, LANES), F32),
            vmem((TILES, 2, LANES), I32),
            vmem((3, SCANS_DEV * TARGET_PTS), F32),
            vmem((3, SCANS_DEV * TARGET_PTS), F32),
            vmem((2, TILES), I32),
            pltpu.SMEM((2, TILES), I32),
            vmem((SCANS_DEV * 4 * 8 + 32, LANES), F32),
            vmem((3 * SCANS_DEV, 6 * TARGET_PTS), jnp.bfloat16),
            vmem((32, 6 * TARGET_PTS), F32),
            vmem((TILES * 16, LANES), F32),
            vmem((TILES * 16, LANES), F32),
            vmem((TILES * 16 + 16, LANES), F32),
            vmem((TILES, LANES), F32),
            vmem((TILES, LANES), F32),
            vmem((TILES, 1, LANES), F32),
            vmem((TILES, 1, LANES), F32),
            vmem((32, LANES), F32),
            vmem((32, LANES), F32),
            pltpu.SemaphoreType.REGULAR,
            dma((6,)),
            dma,
            dma,
            dma((16,)),
            dma,
            dma((16,)),
            dma,
            dma,
            dma,
            dma,
        ],
        compiler_params=pltpu.CompilerParams(collective_id=0, has_side_effects=True, vmem_limit_bytes=56480000),
    )(
        intersection.reshape(1, TILES),
        target_scan,
        source_points.reshape(3 * TILES, 2, LANES),
        matches.reshape(TILES, 2, LANES),
        target_points,
        target_normals,
    )
    return steps[:6, :SCANS_DEV]


def solution(mesh):
    in_specs = (
        P("grp", None, "tile"),
        P("grp", "tile", None),
        P("grp", "tile"),
        P("grp", "tile"),
        P(None, "tile"),
        P(None, "tile"),
    )
    return jax.shard_map(body, mesh=mesh, in_specs=in_specs, out_specs=P(None, "tile"), check_vma=False)
```

```python
import jax
import jax.numpy as jnp
from jax import lax
from jax.experimental import pallas as pl
from jax.experimental.pallas import tpu as pltpu
from jax.sharding import PartitionSpec as P

TILES = 128
SCANS_DEV = 64
TARGET_PTS = 512
LANES = 128
DAMPING = 0.1
PRECISE = lax.Precision.HIGHEST
F32 = jnp.float32
I32 = jnp.int32
DZ_ORDER = (4, 3, 5, 2, 6, 1, 7, 0)
PLANE = 16

PAIRS = [(i, j) for i in range(3) for j in range(i, 3)]
AT_AN, AT_AM, AT_NN, AT_NM, AT_B = 6, 15, 18, 24, 32


def parts_of(value):
    high = value.astype(jnp.bfloat16)
    rest = value - high.astype(F32)
    middle = rest.astype(jnp.bfloat16)
    low = (rest - middle.astype(F32)).astype(jnp.bfloat16)
    return high, middle, low


def solve_rows(rows):
    entries = [[None] * 6 for _ in range(6)]
    for at, (i, j) in enumerate(PAIRS):
        entries[i][j] = entries[j][i] = rows[at]
        entries[3 + i][3 + j] = entries[3 + j][3 + i] = rows[AT_NN + at]
    for i in range(3):
        for j in range(3):
            entries[i][3 + j] = entries[3 + j][i] = rows[AT_AN + 3 * i + j]
    traced = entries[0][0]
    for at in range(1, 6):
        traced = traced + entries[at][at]
    shift_by = DAMPING * traced / 6.0
    for at in range(6):
        entries[at][at] = entries[at][at] + shift_by
    values = [-rows[AT_AM + i] for i in range(3)] + [-rows[AT_NM + i] for i in range(3)]
    for pivot in range(6):
        for row in range(pivot + 1, 6):
            factor = entries[row][pivot] / entries[pivot][pivot]
            for col in range(pivot + 1, 6):
                entries[row][col] = entries[row][col] - factor * entries[pivot][col]
            values[row] = values[row] - factor * values[pivot]
    result = [None] * 6
    for row in range(5, -1, -1):
        running = values[row]
        for col in range(row + 1, 6):
            running = running - entries[row][col] * result[col]
        result[row] = running / entries[row][row]
    return result


def cross(u, v):
    return [u[1] * v[2] - u[2] * v[1], u[2] * v[0] - u[0] * v[2], u[0] * v[1] - u[1] * v[0]]


def turn(at):
    return (2 + 3 * at + 3 * ((at * (at - 1)) // 2)) % 4


def kernel(
    dest_hbm, scan_hbm, src_hbm, mat_hbm, tp_hbm, tn_hbm, out_ref,
    dest_v, scan_s, src_v, mat_v, tp_v, tn_v, inv_v, inv_s, table, rhs, held,
    send, relay, recv, ucat, sums, ret_send, ret_recv, total, total_far,
    ready_sem, in_sem, inv_sem, send_sem, relay_sem, onward_sem, recv_sem,
    ret_ssem, ret_rsem, far_ssem, far_rsem,
):
    me_grp, me = lax.axis_index("grp"), lax.axis_index("tile")
    z, y, x = me // PLANE, (me // 4) % 4, me % 4
    level = me - me % PLANE
    spot = me % PLANE

    def in_plane(group, sign):
        half = group // 8
        dx = turn((1 - half) * (group // 2) + half * (group % 4))
        dy = (1 - half) * (2 + group % 2) + half * (3 - group // 4)
        return level + ((y + 4 + sign * dy) % 4) * 4 + (x + 4 + sign * dx) % 4

    def along_z(dz):
        return ((z + dz) % 8) * PLANE + spot

    copies = [
        pltpu.make_async_copy(s, d, in_sem.at[i])
        for i, (s, d) in enumerate(
            [(dest_hbm, dest_v), (scan_hbm, scan_s), (src_hbm, src_v), (mat_hbm, mat_v), (tp_hbm, tp_v), (tn_hbm, tn_v)]
        )
    ]
    for copy in copies:
        copy.start()

    x_peers = [level + y * 4 + (x + at) % 4 for at in (2, 1, 3)]
    y_peers = [level + ((y + at) % 4) * 4 + x for at in (2, 1, 3)]
    barrier = pltpu.get_barrier_semaphore()
    for peer in [along_z(dz) for dz in DZ_ORDER[:-1]] + y_peers + x_peers:
        pl.semaphore_signal(barrier, 1, device_id={"tile": peer})
    pl.semaphore_signal(barrier, 1, device_id={"grp": 1 - me_grp})

    copies[0].wait()
    blocks = jnp.broadcast_to(dest_v[...], (LANES, LANES)).T
    lane = lax.broadcasted_iota(I32, (LANES, LANES), 1)
    number = lax.broadcasted_iota(I32, (LANES, LANES), 0)
    named = blocks == lane
    first = jnp.min(jnp.where(named, number, 1000), axis=0, keepdims=True)
    last = jnp.max(jnp.where(named, number, -1), axis=0, keepdims=True)
    first = jnp.where(last < 0, -1, first)
    last = jnp.where(last == first, -1, last)
    inv_v[...] = jnp.concatenate([first, last], axis=0)
    to_smem = pltpu.make_async_copy(inv_v, inv_s, inv_sem)
    to_smem.start()
    for copy in copies[1:4]:
        copy.wait()
    to_smem.wait()

    def pack(group, carry):
        place = in_plane(group, 1) % PLANE
        for j, dz in enumerate(DZ_ORDER):
            d = ((z + dz) % 8) * PLANE + place
            slots = send.at[pl.ds(pl.multiple_of(group * LANES, LANES) + j * 16, 16)]
            for r in range(2):
                l = inv_s[r, d]
                block = jnp.minimum(jnp.maximum(l, 0), TILES - 1)
                scale = jnp.where(l >= 0, 1, 0)
                base = jnp.where(l >= 0, scan_s[0, block] * TARGET_PTS, -1)
                for c in range(3):
                    slots[r * 8 + 2 * c : r * 8 + 2 * c + 2, :] = src_v[c * TILES + block]
                slots[r * 8 + 6 : r * 8 + 8, :] = (mat_v[block] * scale + base).astype(F32)
        return carry

    lax.fori_loop(0, 2, pack, 0, unroll=2)
    pl.semaphore_wait(barrier, 7 + 3 + 3 + 1)
    for peer in x_peers:
        pl.semaphore_signal(ready_sem, 1, device_id={"tile": peer})

    def rows_of(group, j=0, count=8):
        return pl.ds(pl.multiple_of(group * LANES, LANES) + j * 16, count * 16)

    def z_copy(source, target, group, j, sent, sem):
        return pltpu.make_async_remote_copy(
            src_ref=source.at[rows_of(group, j, 1)],
            dst_ref=target.at[rows_of(group, j, 1)],
            send_sem=sent,
            recv_sem=sem.at[group],
            device_id={"tile": along_z(DZ_ORDER[j])},
        )

    def plane_copy(source, target, group, sent, sem):
        return pltpu.make_async_remote_copy(
            src_ref=source.at[rows_of(group)],
            dst_ref=target.at[rows_of(group)],
            send_sem=sent,
            recv_sem=sem.at[group],
            device_id={"tile": in_plane(group, 1)},
        )

    def landed(ref, group, sem, count=8):
        piece = ref.at[rows_of(group, 0, count)]
        return pltpu.make_async_copy(piece, piece, sem.at[group])

    def issue(group, carry):
        for j in range(7):
            z_copy(send, relay, group, j, send_sem, relay_sem).start()
        relay[rows_of(group, 7, 1), :] = send[rows_of(group, 7, 1), :]
        return carry

    def issue_plane(group, carry):
        plane_copy(send, relay, group, send_sem, relay_sem).start()
        return carry

    def pack_and_issue(group, carry):
        pack(group, carry)
        return issue(group, carry)

    lax.fori_loop(0, 2, issue, 0)
    lax.fori_loop(2, 8, pack_and_issue, 0)
    lax.fori_loop(8, 16, pack, 0, unroll=2)
    pl.semaphore_wait(ready_sem, 3)
    lax.fori_loop(8, 15, issue_plane, 0)

    copies[4].wait()
    copies[5].wait()

    def spread(at, carry):
        rows = table.at[pl.ds(pl.multiple_of(at * 8, 8), 8)]
        columns = pl.ds(pl.multiple_of(at * LANES, LANES), LANES)
        rows[0:3, :] = tp_v[:, columns]
        rows[3:6, :] = tn_v[:, columns]
        return carry

    lax.fori_loop(0, 4 * SCANS_DEV, spread, 0, unroll=8)
    for c in range(6):
        for chunk in range(4):
            column = jnp.concatenate(
                [table[pl.ds((s8 * 32 + chunk) * 8 + c, 8, stride=32), :] for s8 in range(8)], axis=0
            )
            at = (c * 4 + chunk) * LANES
            for part, piece in enumerate(parts_of(column)):
                rhs[part * 64 : (part + 1) * 64, at : at + LANES] = piece

    lane8 = lax.broadcasted_iota(I32, (8, LANES), 1)

    def settle(groups):
        batches = [(g, r) for g in range(len(groups)) for r in range(2)]

        def rows(g, r, row):
            return recv[pl.ds(groups[g] * LANES + r * 8 + row, 8, stride=16), :]

        wanted = {(g, r, h): rows(g, r, 6 + h).astype(I32) for g, r in batches for h in range(2)}
        scan = {(g, r): lax.shift_right_arithmetic(wanted[g, r, 0][:, 0:1], 9) for g, r in batches}
        column = lax.broadcasted_iota(I32, (8, 3 * SCANS_DEV), 1) & (SCANS_DEV - 1)
        picks = jnp.concatenate([jnp.where(column == scan[b], 1.0, 0.0) for b in batches], axis=0)
        held[: picks.shape[0], :] = jnp.dot(picks.astype(jnp.bfloat16), rhs[...], preferred_element_type=F32)
        for g in range(len(groups)):
            result = jnp.zeros((8, LANES), F32)
            for r in range(2):
                terms = []
                for h in range(2):
                    inside = wanted[g, r, h] & (LANES - 1)
                    odd = (wanted[g, r, h] & LANES) != 0
                    upper = (wanted[g, r, h] & (2 * LANES)) != 0
                    found = []
                    for c in range(6):
                        got = [
                            jnp.take_along_axis(
                                held[(2 * g + r) * 8 : (2 * g + r) * 8 + 8, (4 * c + q) * LANES : (4 * c + q + 1) * LANES],
                                inside, axis=1, mode="promise_in_bounds",
                            )
                            for q in range(4)
                        ]
                        found.append(jnp.where(upper, jnp.where(odd, got[3], got[2]), jnp.where(odd, got[1], got[0])))
                    p, q, n = [rows(g, r, 2 * c + h) for c in range(3)], found[:3], found[3:]
                    a, b = cross(p, n), cross(q, n)
                    m = n[0] * (p[0] - q[0]) + n[1] * (p[1] - q[1]) + n[2] * (p[2] - q[2])
                    terms.append((a, b, n, [m]))

                def put(result, at, left, i, right, j, sign=1):
                    total = terms[0][left][i] * terms[0][right][j] + terms[1][left][i] * terms[1][right][j]
                    value = jnp.sum(total, axis=1, keepdims=True)
                    return jnp.where(lane8 == at + 64 * r, value if sign > 0 else -value, result)

                for at, (i, j) in enumerate(PAIRS):
                    result = put(result, at, 0, i, 0, j)
                    result = put(result, AT_NN + at, 2, i, 2, j)
                    result = put(result, AT_B + at, 1, i, 1, j)
                for i in range(3):
                    for j in range(3):
                        result = put(result, AT_AN + 3 * i + j, 0, i, 2, j)
                        result = put(result, AT_B + AT_AN + 3 * i + j, 1, i, 2, j)
                    result = put(result, AT_AM + i, 0, i, 3, 0)
                    result = put(result, AT_NM + i, 2, i, 3, 0)
                    result = put(result, AT_B + AT_AM + i, 1, i, 3, 0, -1)
            which = jnp.where(lane8 < 64, scan[g, 0], scan[g, 1])
            block = pl.ds(pl.multiple_of(groups[g] * 8, 8), 8)
            ucat[block, :] = jnp.where((lane8 & 63) == which, 1.0, 0.0)
            sums[block, :] = result
            for i in range(8):
                ret_send[groups[g] * 8 + i] = result[i : i + 1, :]

    def back_copy(group, j):
        to = ((z + 8 - DZ_ORDER[j]) % 8) * PLANE + in_plane(group, -1) % PLANE
        return pltpu.make_async_remote_copy(
            src_ref=ret_send.at[group * 8 + j],
            dst_ref=ret_recv.at[me],
            send_sem=ret_ssem,
            recv_sem=ret_rsem,
            device_id={"tile": to},
        )

    def give_back(group, count=8):
        for j in range(count):
            back_copy(group, j).start()

    def onward(step):
        landed(relay, step, relay_sem, 7).wait()
        plane_copy(relay, recv, step, onward_sem, recv_sem).start()

    def onward_z(group):
        landed(relay, group, relay_sem).wait()
        for j in range(7):
            z_copy(relay, recv, group, j, onward_sem, recv_sem).start()
        recv[rows_of(group, 7, 1), :] = relay[rows_of(group, 7, 1), :]

    def early(step, carry):
        onward(step)
        onward_z(step + 8)
        return carry

    def late(step, carry):
        landed(recv, step + 1, recv_sem).wait()
        landed(recv, step + 8, recv_sem, 7).wait()
        settle([step + 1, step + 8])
        give_back(step + 1)
        give_back(step + 8)
        return carry

    lax.fori_loop(0, 7, early, 0)
    onward(7)
    for j in range(7):
        z_copy(send, recv, 15, j, send_sem, recv_sem).start()
    recv[rows_of(15, 7, 1), :] = send[rows_of(15, 7, 1), :]
    landed(recv, 0, recv_sem).wait()
    settle([0])
    give_back(0)
    lax.fori_loop(0, 7, late, 0)
    landed(recv, 15, recv_sem, 7).wait()
    settle([15])
    give_back(15, 7)
    ret_recv[me] = ret_send[15 * 8 + 7]

    by_target = jnp.dot(ucat[...].T, sums[...], precision=PRECISE, preferred_element_type=F32)
    by_target = by_target[:64] + pltpu.roll(by_target[64:], 64, axis=1)
    lane64 = lax.broadcasted_iota(I32, (SCANS_DEV, LANES), 1)
    moved = pltpu.roll(by_target, LANES - AT_B, axis=1)
    by_target = jnp.where(
        lane64 < AT_NN, moved, jnp.where(lane64 < AT_NM, by_target, jnp.where(lane64 < AT_NM + 3, -by_target, 0.0))
    )
    scan_row = lax.broadcasted_iota(I32, (SCANS_DEV, LANES), 0)
    owner = [lax.shift_right_arithmetic(inv_v[r : r + 1, :], 1) for r in range(2)]
    scat = jnp.concatenate([jnp.where(scan_row == owner[r], 1.0, 0.0) for r in range(2)], axis=0)

    sent = send.at[pl.ds(0, 8 * 7 * 16 + 7 * 8 * 16 + 7 * 16)]
    pltpu.make_async_copy(sent, sent, send_sem).wait()
    moved_on = relay.at[pl.ds(0, 8 * 8 * 16 + 7 * 7 * 16)]
    pltpu.make_async_copy(moved_on, moved_on, onward_sem).wait()
    others = ret_recv.at[pl.ds(0, TILES - 1)]
    pltpu.make_async_copy(others, others, ret_rsem).wait()
    gone = ret_send.at[pl.ds(0, TILES - 1)]
    pltpu.make_async_copy(gone, gone, ret_ssem).wait()
    returned = ret_recv[...].reshape(TILES, LANES)
    by_source = jnp.dot(scat, returned, precision=PRECISE, preferred_element_type=F32)
    by_source = by_source[:64] + pltpu.roll(by_source[64:], 64, axis=1)
    both = by_source + by_target
    flipped = jnp.concatenate([both, jnp.zeros_like(both)], axis=0).T
    total[...] = flipped[:32, :]
    far = pltpu.make_async_remote_copy(
        src_ref=total, dst_ref=total_far, send_sem=far_ssem, recv_sem=far_rsem, device_id={"grp": 1 - me_grp}
    )
    far.start()
    far.wait_recv()
    whole = total[...] + total_far[...]
    result = solve_rows([whole[at : at + 1, :] for at in range(27)])
    for row in range(6):
        out_ref[row : row + 1, :] = result[row]
    far.wait_send()


def body(source_points, intersection, target_scan, matches, target_points, target_normals):
    anywhere = pl.BlockSpec(memory_space=pl.ANY)
    vmem = pltpu.VMEM
    dma = pltpu.SemaphoreType.DMA
    steps = pl.pallas_call(
        kernel,
        name="icp_step",
        out_shape=jax.ShapeDtypeStruct((8, LANES), F32),
        in_specs=[anywhere] * 6,
        out_specs=pl.BlockSpec(memory_space=pltpu.VMEM),
        scratch_shapes=[
            vmem((1, TILES), I32),
            pltpu.SMEM((1, TILES), I32),
            vmem((3 * TILES, 2, LANES), F32),
            vmem((TILES, 2, LANES), I32),
            vmem((3, SCANS_DEV * TARGET_PTS), F32),
            vmem((3, SCANS_DEV * TARGET_PTS), F32),
            vmem((2, TILES), I32),
            pltpu.SMEM((2, TILES), I32),
            vmem((SCANS_DEV * 4 * 8 + 32, LANES), F32),
            vmem((3 * SCANS_DEV, 6 * TARGET_PTS), jnp.bfloat16),
            vmem((32, 6 * TARGET_PTS), F32),
            vmem((TILES * 16, LANES), F32),
            vmem((TILES * 16, LANES), F32),
            vmem((TILES * 16 + 16, LANES), F32),
            vmem((TILES, LANES), F32),
            vmem((TILES, LANES), F32),
            vmem((TILES, 1, LANES), F32),
            vmem((TILES, 1, LANES), F32),
            vmem((32, LANES), F32),
            vmem((32, LANES), F32),
            pltpu.SemaphoreType.REGULAR,
            dma((6,)),
            dma,
            dma,
            dma((16,)),
            dma,
            dma((16,)),
            dma,
            dma,
            dma,
            dma,
        ],
        compiler_params=pltpu.CompilerParams(collective_id=0, has_side_effects=True, vmem_limit_bytes=56480000),
    )(
        intersection.reshape(1, TILES),
        target_scan,
        source_points.reshape(3 * TILES, 2, LANES),
        matches.reshape(TILES, 2, LANES),
        target_points,
        target_normals,
    )
    return steps[:6, :SCANS_DEV]


def solution(mesh):
    in_specs = (
        P("grp", None, "tile"),
        P("grp", "tile", None),
        P("grp", "tile"),
        P("grp", "tile"),
        P(None, "tile"),
        P(None, "tile"),
    )
    return jax.shard_map(body, mesh=mesh, in_specs=in_specs, out_specs=P(None, "tile"), check_vma=False)
```
